256 devices in a mesh: branch: 2 (over z_lo), batch: 32 (over y, z_hi, core), rows: 4 (over x).
Axes of the slice: x: 4, y: 4, z: 8 (z_hi: 4, z_lo: 2; z = z_hi * 2 + z_lo), core: 2. Of those that a mesh axis runs over, the one named last changes fastest.
Arguments:
- timestep: int32 [32], P('batch'), parts along dimension 0, may hold values from 0 to 999
- features: bfloat16 [32, 2, 32, 64, 640], P('batch', 'branch', 'rows'), parts along dimension 0, may hold values from -6 to 6
- conv1_weight: bfloat16 [2, 3, 3, 640, 640], P('branch', None, None, None, 'rows'), may hold values from -0.078125 to 0.078125
- conv1_bias: float32 [2, 640], P('branch'), may hold values from -3 to 3
- conv2_weight: bfloat16 [2, 3, 3, 640, 640], P('branch', None, None, None, 'rows'), may hold values from -0.078125 to 0.078125
- conv2_bias: float32 [2, 640], P('branch'), may hold values from -3 to 3
- norm1_gain: float32 [2, 640], P('branch'), may hold values from 0.25 to 1.75
- norm1_shift: float32 [2, 640], P('branch'), may hold values from -3 to 3
- norm2_gain: float32 [2, 640], P('branch'), may hold values from 0.25 to 1.75
- norm2_shift: float32 [2, 640], P('branch'), may hold values from -3 to 3
- time_weight: bfloat16 [2, 320, 1280], P('branch'), may hold values from -0.3125 to 0.3125
- emb_weight: bfloat16 [2, 1280, 640], P('branch'), may hold values from -0.15625 to 0.15625
- zero_weight: bfloat16 [640, 640], replicated, may hold values from -0.25 to 0.25
- zero_bias: float32 [640], replicated, may hold values from -3 to 3
Outputs:
- block_out: bfloat16 [32, 2, 32, 64, 640], P('batch', 'branch', 'rows'), parts along dimension 0
The draws below stay inside these ranges and needn't reach their ends.
There are 32 independent parts, one for each index of `batch`. The reference program is written for one: setup_inputs(seed, part) draws one part's arguments, and reference() takes and returns one part's arrays. A program takes and returns all parts, laid end to end along the dimension named above; an argument that names none is the same for every part. Nothing has to cross between parts.
All inputs are finite; a program needn't handle non-finite values.
Results may differ from the reference program's by a relative error of at most 0.01.
Values may be sent and summed in bfloat16 or wider, within the bound.
A program may use at most 128 MiB of HBM per device.

```python
import math
import jax
import jax.numpy as jnp
from jax import lax

C = 640
GROUPS = 32
TEMB = 1280
TFREQ = 320
WIDTH = 64
HEIGHT = 32


def levels(stream_key, extent, pieces, low, largest):
    factor_of, own = 1.0, jax.random.fold_in(stream_key, 6)
    for dim, parts in pieces:
        heights = jnp.exp(jax.random.uniform(jax.random.fold_in(own, dim), (parts,), jnp.float32, low / len(pieces), largest / len(pieces)))
        factor_of = factor_of * jnp.repeat(heights, extent[dim] // parts).reshape([-1 if axis == dim else 1 for axis in range(len(extent))])
    return factor_of


def scatter_about(key, shape, scale, bound, pieces=(), kind=jnp.bfloat16):
    array = jax.random.normal(key, shape, jnp.float32) * scale
    if len(pieces) > 0:
        array = levels(key, shape, pieces, -0.22, 0.18) * array
    return jnp.clip(array, min=-bound, max=bound).astype(kind)


def setup_inputs(seed: int = 0, part: int = 0) -> dict:
    streams_of = jax.random.split(jax.random.key(seed), 15)
    part_keys = jax.random.split(jax.random.fold_in(streams_of[14], part), 15)
    timestep = jax.random.randint(part_keys[0], (1,), 0, 1000).astype(jnp.int32)
    features = scatter_about(part_keys[1], (1, 2, HEIGHT, WIDTH, C), 1.0, 6.0, ((1, 2), (2, 4)))
    conv1_weight = scatter_about(streams_of[2], (2, 3, 3, C, C), (9 * C) ** -0.5, 0.078125, ((0, 2), (4, 4)))
    conv1_bias = scatter_about(streams_of[3], (2, C), 0.5, 3.0, ((0, 2),), jnp.float32)
    conv2_weight = scatter_about(streams_of[4], (2, 3, 3, C, C), (9 * C) ** -0.5, 0.078125, ((0, 2), (4, 4)))
    conv2_bias = scatter_about(streams_of[5], (2, C), 0.5, 3.0, ((0, 2),), jnp.float32)
    norm1_gain = jnp.clip(1.0 + 0.15 * jax.random.normal(streams_of[6], (2, C), jnp.float32), 0.25, 1.75)
    norm1_shift = scatter_about(streams_of[7], (2, C), 0.5, 3.0, ((0, 2),), jnp.float32)
    norm2_gain = jnp.clip(1.0 + 0.15 * jax.random.normal(streams_of[8], (2, C), jnp.float32), 0.25, 1.75)
    norm2_shift = scatter_about(streams_of[9], (2, C), 0.5, 3.0, ((0, 2),), jnp.float32)
    time_weight = scatter_about(streams_of[10], (2, TFREQ, TEMB), TFREQ ** -0.5, 0.3125, ((0, 2),))
    emb_weight = scatter_about(streams_of[11], (2, TEMB, C), TEMB ** -0.5, 0.15625, ((0, 2),))
    zero_weight = scatter_about(streams_of[12], (C, C), C ** -0.5, 0.25)
    zero_bias = scatter_about(streams_of[13], (C,), 0.5, 3.0, (), jnp.float32)
    return {"timestep": timestep, "features": features, "conv1_weight": conv1_weight, "conv1_bias": conv1_bias, "conv2_weight": conv2_weight, "conv2_bias": conv2_bias, "norm1_gain": norm1_gain, "norm1_shift": norm1_shift, "norm2_gain": norm2_gain, "norm2_shift": norm2_shift, "time_weight": time_weight, "emb_weight": emb_weight, "zero_weight": zero_weight, "zero_bias": zero_bias}


def sinusoid(timestep, count):
    half = count // 2
    freqs = jnp.exp(-math.log(10000.0) * jnp.arange(half, dtype=jnp.float32) / half)
    angles = timestep.astype(jnp.float32)[0] * freqs
    return jnp.concatenate([jnp.cos(angles), jnp.sin(angles)])

def time_shift(timestep, time_weight, emb_weight):
    waves = sinusoid(timestep, time_weight.shape[0])
    inner = jax.nn.silu(jnp.dot(waves, time_weight.astype(jnp.float32), precision=lax.Precision.HIGHEST))
    return jnp.dot(inner, emb_weight.astype(jnp.float32), precision=lax.Precision.HIGHEST)

def group_norm(values, gain, shift):
    rows, cols, chans = values.shape
    grouped = values.reshape(rows, cols, GROUPS, chans // GROUPS)
    mean = lax.optimization_barrier(jnp.mean(grouped, axis=(0, 1, 3)))
    var = lax.optimization_barrier(jnp.mean(grouped * grouped, axis=(0, 1, 3))) - mean * mean
    normed = (grouped - mean[:, None]) * lax.rsqrt(var + 1e-05)[:, None]
    return jax.nn.silu(normed.reshape(values.shape) * gain + shift).astype(jnp.bfloat16)

def convolve(inputs, kernel):
    return lax.conv_general_dilated(inputs[None], kernel, (1, 1), 'SAME', dimension_numbers=('NHWC', 'HWIO', 'NHWC'), preferred_element_type=jnp.float32)[0]

def reference(timestep, features, conv1_weight, conv1_bias, conv2_weight, conv2_bias, norm1_gain, norm1_shift, norm2_gain, norm2_shift, time_weight, emb_weight, zero_weight, zero_bias):
    blocks = []
    for which in range(2):
        inputs = features[0, which]
        extra = time_shift(timestep, time_weight[which], emb_weight[which])
        act = group_norm(inputs.astype(jnp.float32), norm1_gain[which], norm1_shift[which])
        hidden = (convolve(act, conv1_weight[which]) + conv1_bias[which] + extra).astype(jnp.bfloat16)
        act_two = group_norm(hidden.astype(jnp.float32), norm2_gain[which], norm2_shift[which])
        blocks.append(inputs.astype(jnp.float32) + convolve(act_two, conv2_weight[which]) + conv2_bias[which])
    control_out = blocks[0].astype(jnp.bfloat16)
    flat = control_out.reshape(-1, control_out.shape[2])
    control_res = (jnp.dot(flat, zero_weight, preferred_element_type=jnp.float32) + zero_bias).astype(jnp.bfloat16)
    base_out = (blocks[1] + control_res.reshape(control_out.shape).astype(jnp.float32)).astype(jnp.bfloat16)
    return jnp.stack([control_out, base_out])[None]
```

```python
import functools
import math

import numpy as np

import jax
import jax.numpy as jnp
from jax import lax
from jax.experimental import pallas as pl
from jax.experimental.pallas import tpu as pltpu
from jax.sharding import PartitionSpec as P

C = 640
GROUP = 20
W = 64
HR = 8
POS = HR * W
TAPS = 5760
QC = 160
EDGE = 720
CUT = 368
REST = 1440
COUNT = 2048 * GROUP
MESH = pl.DeviceIdType.MESH
F32 = jnp.float32
BF16 = jnp.bfloat16


def chan_of(p):
    r = p - 512
    return jnp.where(p < 512, (p >> 7) * QC + (p & 127), (r >> 5) * QC + 128 + (r & 31))


def group_of(c):
    return (c * 3277) >> 16


def iota(shape, dim):
    return lax.broadcasted_iota(jnp.int32, shape, dim)


def split3(x):
    hi = x.astype(BF16).astype(F32)
    left = x - hi
    mid = left.astype(BF16).astype(F32)
    return jnp.concatenate([hi, mid, left - mid], axis=0).astype(BF16)


def exact_dot(x, m):
    out = jnp.dot(split3(x), m, preferred_element_type=F32)
    return out[0:8] + out[8:16] + out[16:24]


def silu(x):
    h = 0.5 * x
    return h + h * jnp.tanh(h)


class Links:
    def __init__(self, send, recv):
        self.send, self.recv = send, recv
        self.keys, self.started, self.count = {}, [], 0

    def slot(self, key):
        return self.keys.setdefault(key, len(self.keys))

    def put(self, key, src, dst, device):
        copy = pltpu.make_async_remote_copy(
            src_ref=src,
            dst_ref=dst,
            send_sem=self.send.at[self.count],
            recv_sem=self.recv.at[self.slot(key)],
            device_id=device,
            device_id_type=MESH,
        )
        self.count += 1
        copy.start()
        self.started.append(copy)
        return copy

    def get(self, key, dst, device):
        pltpu.make_async_remote_copy(
            src_ref=dst,
            dst_ref=dst,
            send_sem=self.send.at[0],
            recv_sem=self.recv.at[self.slot(key)],
            device_id=device,
            device_id_type=MESH,
        ).wait_recv()

    def drain(self):
        for copy in self.started:
            copy.wait_send()


def kernel(
    ts, freq, feats, w1, w2, b1, b2, g1, s1, g2, s2, tw, ew, zw, zb,
    out,
    src, hid, xcat, acc, basep, ctl, wm, pk, wr, own,
    group_nat, group_til, perm, perm_t, pack, spread, stats, vin, vecs, twv, ewv, zwv, zp, fr, outv,
    lsem, send, recv,
):
    x = lax.axis_index("rows")
    b = lax.axis_index("batch")
    branch = lax.axis_index("branch")
    core = b % 2
    zh = (b // 2) % 4
    y = b // 8
    label = (y + 2 * zh) % 4

    def along_x(by):
        return {"rows": (x + by) % 4}

    def along_batch(ny, nz, nc):
        return {"batch": (ny * 4 + nz) * 2 + nc}

    right, left, across = along_x(1), along_x(3), along_x(2)
    up, down = along_batch((y + 1) % 4, zh, core), along_batch((y + 3) % 4, zh, core)
    front, back = along_batch(y, (zh + 1) % 4, core), along_batch(y, (zh + 3) % 4, core)
    twin = along_batch(y, zh, 1 - core)
    mate = {"branch": 1 - branch}

    barrier = pltpu.get_barrier_semaphore()
    for device in (right, left, across, up, down, front, back, twin, mate):
        pl.semaphore_signal(barrier, inc=1, device_id=device, device_id_type=MESH)

    local = {}

    def load(name, a, to):
        copy = pltpu.make_async_copy(a, to, lsem.at[len(local)])
        copy.start()
        local[name] = copy

    weights = (w1, w2)
    load("feats", feats, src.at[pl.ds(W, POS), :])
    load("own0", w1, own.at[0])
    load("own1", w2, own.at[1])
    load("main0", w1.at[:, pl.ds(0, 128)], wm.at[0, x])
    load("main1", w2.at[:, pl.ds(0, 128)], wm.at[1, x])
    load("fr", freq, fr)
    for i, ref in enumerate((b1, b2, g1, s1, g2, s2, zb)):
        load(f"vec{i}", ref, vin.at[i])
    load("tw", tw, twv)
    load("ew", ew, ewv)
    load("zw", zw, zwv)

    pl.semaphore_wait(barrier, 9)
    net = Links(send, recv)

    quarter = {"own": x, "L": (x + 3) % 4, "R": (x + 1) % 4, "F": (x + 2) % 4}
    span = {"A": (0, CUT), "B": (CUT, EDGE - CUT), "AB": (0, EDGE)}

    def piece(v, rel, p, c, part):
        first, size = span[part]
        return wm.at[v, quarter[rel], pl.ds(pl.multiple_of(EDGE * (2 * p + c) + first, 16), size), :]

    def rest(v, rel, c, part):
        first, size = span[part]
        return pk.at[v, quarter[rel], pl.ds(pl.multiple_of(EDGE * c + first, 16), size), :]

    def send_own(v):
        for part in "AB":
            first, size = span[part]
            row = pl.multiple_of(EDGE * (2 * label + core) + first, 16)
            a = weights[v].at[pl.ds(row, size), pl.ds(0, 128)]
            to = piece(v, "own", label, core, part)
            net.put((v, "L", part), a, to, right)
            net.put((v, "R", part), a, to, left)

    def send_rest(v):
        a = rest(v, "own", core, "AB")
        net.put((v, "L", "C"), a, a, right)
        net.put((v, "R", "C"), a, a, left)

    def on_piece(v, rel, part):
        ref = piece(v, rel, label, core, part)
        if rel == "F":
            came = left if part == "A" else right
        else:
            came = left if rel == "L" else right
        net.get((v, rel, part), ref, came)
        net.put((v, "Yd", rel, part), ref, ref, up)
        net.put((v, "Yu", rel, part), ref, ref, down)
        net.put((v, "Z", rel, part), ref, ref, front if part == "A" else back)
        if rel == "L" and part == "A":
            net.put((v, "F", "A"), ref, ref, right)
        if rel == "R" and part == "B":
            net.put((v, "F", "B"), ref, ref, left)

    def on_rest(v, rel):
        ref = rest(v, rel, core, "AB")
        net.get((v, rel, "C"), ref, left if rel == "L" else right)
        part = "A" if rel == "L" else "B"
        half = rest(v, rel, core, part)
        net.put((v, "F", "C" + part), half, half, right if rel == "L" else left)
        net.put((v, "S", rel, "C"), ref, ref, twin)

    def on_far_rest(v):
        net.get((v, "F", "CA"), rest(v, "F", core, "A"), left)
        net.get((v, "F", "CB"), rest(v, "F", core, "B"), right)
        ref = rest(v, "F", core, "AB")
        net.put((v, "S", "F", "C"), ref, ref, twin)

    def to_twin(v, rel, step):
        ref = piece(v, rel, (label + step) % 4, core, "AB")
        net.put((v, "S", rel, step), ref, ref, twin)

    def on_side(v, rel, step):
        p = (label + step) % 4
        for part in "AB":
            if step == 2:
                net.get((v, "Z", rel, part), piece(v, rel, p, core, part), back if part == "A" else front)
            elif step == 1:
                net.get((v, "Yu", rel, part), piece(v, rel, p, core, part), up)
            else:
                net.get((v, "Yd", rel, part), piece(v, rel, p, core, part), down)
        to_twin(v, rel, step)

    def from_twin(v, rel):
        for step in range(4):
            net.get((v, "S", rel, step), piece(v, rel, (label + step) % 4, 1 - core, "AB"), twin)

    def rest_from_twin(v, rel):
        net.get((v, "S", rel, "C"), rest(v, rel, 1 - core, "AB"), twin)

    def one_hots():
        for k in range(10):
            rows = pl.ds(64 * k, 64)
            i = iota((64, C), 0) + 64 * k
            j = iota((64, C), 1)
            ci, cj = chan_of(i), chan_of(j)

            def as_matrix(test):
                return jnp.where(test, 1.0, 0.0).astype(BF16)

            group_nat[rows, :] = as_matrix(group_of(i) == group_of(j))
            group_til[rows, :] = as_matrix(group_of(ci) == group_of(cj))
            perm[rows, :] = as_matrix(i == cj)
            perm_t[rows, :] = as_matrix(ci == j)

    def pack_matrices():
        i = iota((QC, 128), 0)
        j = iota((QC, 128), 1)
        for g in range(4):
            pack[g] = jnp.where(i - 128 == j - 32 * g, jnp.where(i >= 128, 1.0, 0.0), 0.0).astype(BF16)
        r = iota((512, 256), 0)
        n = iota((512, 256), 1)
        for h in range(2):
            same = (r >> 7) == ((n & 127) >> 5)
            lane = (r & 31) == (n & 31)
            which = ((r & 127) >> 5) == 2 * h + (n >> 7)
            spread[h] = jnp.where(same & lane & which, 1.0, 0.0).astype(BF16)

    def pack_rest(v):
        def step(k, _):
            row = pl.multiple_of(480 * k, 16)
            total = jnp.zeros((480, 128), F32)
            for g in range(4):
                total += jnp.dot(
                    own[v, pl.ds(row + REST * g, 480), :], pack[g], preferred_element_type=F32
                )
            pk[v, x, pl.ds(row, 480), :] = total.astype(BF16)
            return 0

        lax.fori_loop(0, 3, step, 0)

    def spread_rest(v):
        def step(k, _):
            row = pl.multiple_of(480 * k, 16)
            lhs = jnp.concatenate([pk[v, q, pl.ds(row, 480), :] for q in range(4)], axis=1)
            for h in range(2):
                two = jnp.dot(lhs, spread[h], preferred_element_type=F32).astype(BF16)
                wr[v, pl.ds(row + REST * (2 * h), 480), :] = two[:, :128]
                wr[v, pl.ds(row + REST * (2 * h + 1), 480), :] = two[:, 128:]
            return 0

        lax.fori_loop(0, 3, step, 0)

    def send_stats(k):
        ref = stats.at[k, x]
        for by, device in ((1, right), (2, across), (3, left)):
            net.put(("stats", k, by), ref, ref, device)

    def moments(k, groups):
        for by, device in ((1, left), (2, across), (3, right)):
            net.get(("stats", k, by), stats.at[k, (x - by + 4) % 4], device)
        total = stats[k, 0] + stats[k, 1] + stats[k, 2] + stats[k, 3]
        sums = exact_dot(total, groups[...]) * (1.0 / COUNT)
        mean = sums[0:1]
        var = sums[1:2] - mean * mean
        return mean, lax.rsqrt(var + 1e-05)

    def send_edges(ref, buf, key):
        net.put((key, "top"), ref(POS - W), buf.at[pl.ds(0, W), :], right)
        net.put((key, "end"), ref(0), buf.at[pl.ds(POS + W, W), :], left)

    def wait_edges(buf, key):
        net.get((key, "top"), buf.at[pl.ds(0, W), :], left)
        net.get((key, "end"), buf.at[pl.ds(POS + W, W), :], right)

    def activate(buf, mean, scale, shift):
        def step(i, _):
            rows = pl.ds(pl.multiple_of(W * i, W), W)
            outside = ((i == 0) & (x == 0)) | ((i == 9) & (x == 3))
            keep = jnp.where(outside, 0.0, 1.0)
            v = buf[rows, :].astype(F32)
            a = silu((v - mean) * scale + shift) * keep
            col = iota((W, C), 0)
            xcat[rows, pl.ds(0, C)] = jnp.where(col == 0, 0.0, pltpu.roll(a, 1, 0)).astype(BF16)
            xcat[rows, pl.ds(C, C)] = a.astype(BF16)
            xcat[rows, pl.ds(2 * C, C)] = jnp.where(col == W - 1, 0.0, pltpu.roll(a, W - 1, 0)).astype(BF16)
            return 0

        lax.fori_loop(0, 10, step, 0)

    def rows_of(load_rows, first, tiled):
        if not tiled:
            return load_rows(first, 3 * C)
        parts = []
        for dx in range(3):
            parts += [load_rows(first + dx * C + QC * q, 128) for q in range(4)]
            parts += [load_rows(first + dx * C + QC * q + 128, 32) for q in range(4)]
        return jnp.concatenate(parts, axis=0)

    def conv_pair(v, qa, tiled):
        def step(dy, _):
            first = pl.multiple_of(3 * C * dy, 128)
            lhs = xcat[pl.ds(pl.multiple_of(W * dy, W), POS), :]
            rhs = [
                rows_of(lambda r, n, q=q: wm[v, q, pl.ds(pl.multiple_of(r, 16), n), :], first, tiled)
                for q in (qa, qa + 1)
            ]
            r = jnp.dot(lhs, jnp.concatenate(rhs, axis=1), preferred_element_type=F32)
            acc[qa] += r[:, :128]
            acc[qa + 1] += r[:, 128:]
            return 0

        lax.fori_loop(0, 3, step, 0)

    def conv_rest(v, tiled):
        def step(dy, _):
            first = pl.multiple_of(3 * C * dy, 128)
            lhs = xcat[pl.ds(pl.multiple_of(W * dy, W), POS), :]
            rhs = rows_of(lambda r, n: wr[v, pl.ds(pl.multiple_of(r, 16), n), :], first, tiled)
            acc[4] += jnp.dot(lhs, rhs, preferred_element_type=F32)
            return 0

        lax.fori_loop(0, 3, step, 0)

    def clear():
        for t in range(5):
            acc[t] = jnp.zeros((POS, 128), F32)

    near_pair = 2 * (x // 2)
    far_pair = 2 - near_pair

    send_own(0)
    send_edges(lambda r: feats.at[pl.ds(r, W), :], src, "features")
    pack_matrices()
    local["own0"].wait()
    pack_rest(0)

    local["feats"].wait()

    def sums(i, carry):
        total, square = carry
        v = src[pl.ds(pl.multiple_of(W + 32 * i, 32), 32), :].astype(F32)
        for k in range(4):
            part = v[8 * k : 8 * k + 8]
            total, square = total + part, square + part * part
        return total, square

    def put_stats(k, total, square):
        row = iota((8, C), 0)
        stats[k, x] = jnp.where(
            row == 0,
            jnp.sum(total, axis=0, keepdims=True),
            jnp.where(row == 1, jnp.sum(square, axis=0, keepdims=True), 0.0),
        )

    zero = jnp.zeros((8, C), F32)
    total, square = lax.fori_loop(0, POS // 32, sums, (zero, zero))
    put_stats(0, total, square)
    send_rest(0)
    one_hots()
    send_stats(0)

    on_piece(0, "L", "A")
    on_piece(0, "R", "A")

    for i in range(7):
        local[f"vec{i}"].wait()
    local["fr"].wait()
    local["tw"].wait()
    local["ew"].wait()
    angle = jnp.broadcast_to(fr[...] * ts[0].astype(F32), (8, 320))
    n = jnp.floor(angle * (2.0 / math.pi) + 0.5)
    r = ((angle - n * 1.5703125) - n * 4.837512969970703e-4) - n * 7.549790126404332e-8
    turn = n + jnp.where(iota((8, 320), 1) < 160, 1.0, 0.0)
    turn = turn - 4.0 * jnp.floor(turn * 0.25)
    r2 = r * r
    sin_r = r + r * r2 * (-1.0 / 6 + r2 * (1.0 / 120 + r2 * (-1.0 / 5040 + r2 * (1.0 / 362880))))
    cos_r = 1.0 + r2 * (-0.5 + r2 * (1.0 / 24 + r2 * (-1.0 / 720 + r2 * (1.0 / 40320 - r2 * (1.0 / 3628800)))))
    waves = jnp.where(
        turn < 0.5, sin_r, jnp.where(turn < 1.5, cos_r, jnp.where(turn < 2.5, -sin_r, -cos_r))
    )
    inner = silu(exact_dot(waves, twv[...]))
    extra = exact_dot(inner, ewv[...])
    row = iota((8, C), 0)
    stack = jnp.where(row == 0, vin[0] + extra, 0.0)
    for i, k in ((1, 4), (2, 5), (3, 1), (4, 6)):
        stack = jnp.where(row == i, vin[k], stack)
    vecs[...] = exact_dot(stack, perm[...])

    on_piece(0, "L", "B")
    on_piece(0, "R", "B")

    wait_edges(src, "features")
    mean, scale = moments(0, group_nat)
    activate(src, mean, scale * vin[2], vin[3])

    on_rest(0, "L")
    on_rest(0, "R")
    to_twin(0, "L", 0)
    to_twin(0, "R", 0)
    send_own(1)

    local["own1"].wait()
    pack_rest(1)

    def residual(i, _):
        rows = pl.ds(pl.multiple_of(W + 128 * i, 64), 128)
        r = jnp.dot(src[rows, :], perm[...], preferred_element_type=F32)
        for t in range(5):
            basep[t, pl.ds(pl.multiple_of(128 * i, 128), 128), :] = (
                r[:, 128 * t : 128 * t + 128] + vecs[3:4, 128 * t : 128 * t + 128]
            )
        return 0

    lax.fori_loop(0, 4, residual, 0)
    send_rest(1)

    on_piece(0, "F", "A")
    on_piece(0, "F", "B")
    to_twin(0, "F", 0)

    for rel in "LR":
        for step in (1, 3, 2):
            on_side(0, rel, step)

    local["zw"].wait()
    for t in range(5):
        if t < 4:
            lhs = zwv[pl.ds(QC * t, 128), :]
        else:
            lhs = jnp.concatenate([zwv[pl.ds(QC * q + 128, 32), :] for q in range(4)], axis=0)
        zp[pl.ds(128 * t, 128), :] = jnp.dot(lhs, perm[...], preferred_element_type=F32).astype(BF16)

    on_far_rest(0)
    for rel in "LRF":
        rest_from_twin(0, rel)
    spread_rest(0)
    clear()
    conv_rest(0, False)

    local["main0"].wait()
    for rel in "LR":
        from_twin(0, rel)
    on_piece(1, "L", "A")
    on_piece(1, "R", "A")
    conv_pair(0, near_pair, False)

    on_piece(1, "L", "B")
    on_piece(1, "R", "B")
    for step in (1, 3, 2):
        on_side(0, "F", step)
    on_rest(1, "L")
    on_rest(1, "R")
    to_twin(1, "L", 0)
    to_twin(1, "R", 0)
    from_twin(0, "F")
    conv_pair(0, far_pair, False)

    on_piece(1, "F", "A")
    on_piece(1, "F", "B")
    to_twin(1, "F", 0)

    def hidden(i, carry):
        carry = list(carry)
        rows = pl.ds(pl.multiple_of(W * i, W), W)
        for t in range(5):
            h = (acc[t, rows, :] + vecs[0:1, 128 * t : 128 * t + 128]).astype(BF16)
            hid[pl.ds(pl.multiple_of(W + W * i, W), W), pl.ds(128 * t, 128)] = h
            h = h.astype(F32)
            for k in range(8):
                part = h[8 * k : 8 * k + 8]
                carry[2 * t] = carry[2 * t] + part
                carry[2 * t + 1] = carry[2 * t + 1] + part * part
        return tuple(carry)

    zero = jnp.zeros((8, 128), F32)
    carry = lax.fori_loop(0, HR, hidden, (zero,) * 10)
    put_stats(1, jnp.concatenate(carry[0::2], axis=1), jnp.concatenate(carry[1::2], axis=1))
    send_edges(lambda r: hid.at[pl.ds(W + r, W), :], hid, "hidden")
    clear()
    send_stats(1)
    for rel in "LR":
        for step in (1, 3, 2):
            on_side(1, rel, step)
    on_far_rest(1)
    for rel in "LRF":
        rest_from_twin(1, rel)
    spread_rest(1)
    wait_edges(hid, "hidden")
    mean, scale = moments(1, group_til)
    activate(hid, mean, scale * vecs[1:2, :], vecs[2:3, :])

    def ctl_out(t):
        @pl.when(branch == 0)
        def _():
            ctl[t] = (acc[t] + basep[t]).astype(BF16)

    def ctl_put(slot, t):
        copy = pltpu.make_async_remote_copy(
            src_ref=ctl.at[t],
            dst_ref=ctl.at[t],
            send_sem=send.at[slot],
            recv_sem=recv.at[slot],
            device_id=mate,
            device_id_type=MESH,
        )
        return copy

    base_slot = 100
    order = [4, near_pair, near_pair + 1, far_pair, far_pair + 1]

    def give(k):
        ctl_out(order[k])

        @pl.when(branch == 0)
        def _():
            ctl_put(base_slot + k, order[k]).start()

    conv_rest(1, True)
    give(0)
    local["main1"].wait()
    for rel in "LR":
        from_twin(1, rel)
    conv_pair(1, near_pair, True)
    give(1)
    give(2)
    for step in (1, 3, 2):
        on_side(1, "F", step)
    from_twin(1, "F")
    conv_pair(1, far_pair, True)
    give(3)
    give(4)

    @pl.when(branch == 1)
    def _():
        for k in range(5):
            ctl_put(base_slot + k, order[k]).wait_recv()

        def step(i, _):
            rows = pl.ds(pl.multiple_of(128 * i, 128), 128)
            lhs = jnp.concatenate([ctl[t, rows, :] for t in range(5)], axis=1)
            res = jnp.dot(lhs, zp[...], preferred_element_type=F32) + vecs[4:5, :]
            res = res.astype(BF16).astype(F32)
            for t in range(5):
                pre = acc[t, rows, :] + basep[t, rows, :]
                ctl[t, rows, :] = (pre + res[:, 128 * t : 128 * t + 128]).astype(BF16)
            return 0

        lax.fori_loop(0, 4, step, 0)

    def natural(i, _):
        rows = pl.ds(pl.multiple_of(128 * i, 128), 128)
        lhs = jnp.concatenate([ctl[t, rows, :] for t in range(5)], axis=1)
        outv[rows, :] = jnp.dot(lhs, perm_t[...], preferred_element_type=F32).astype(BF16)
        return 0

    lax.fori_loop(0, 4, natural, 0)
    done = pltpu.make_async_copy(outv, out, lsem.at[len(local)])
    done.start()

    @pl.when(branch == 0)
    def _():
        for k in range(5):
            ctl_put(base_slot + k, order[k]).wait_send()

    net.drain()
    done.wait()


def body(
    timestep,
    features,
    conv1_weight,
    conv1_bias,
    conv2_weight,
    conv2_bias,
    norm1_gain,
    norm1_shift,
    norm2_gain,
    norm2_shift,
    time_weight,
    emb_weight,
    zero_weight,
    zero_bias,
):
    half = 160
    line = np.exp(-math.log(10000.0) * np.arange(half, dtype=np.float32) / np.float32(half))
    freq = jnp.asarray(np.concatenate([line, line])[None].astype(np.float32))
    hbm = pl.BlockSpec(memory_space=pltpu.HBM)
    vmem = pltpu.VMEM
    result = pl.pallas_call(
        kernel,
        out_shape=jax.ShapeDtypeStruct((POS, C), BF16),
        in_specs=[pl.BlockSpec(memory_space=pltpu.SMEM)] + [hbm] * 14,
        out_specs=hbm,
        scratch_shapes=[
            vmem((POS + 2 * W, C), BF16),
            vmem((POS + 2 * W, C), BF16),
            vmem((POS + 2 * W, 3 * C), BF16),
            vmem((5, POS, 128), F32),
            vmem((5, POS, 128), F32),
            vmem((5, POS, 128), BF16),
            vmem((2, 4, TAPS, 128), BF16),
            vmem((2, 4, REST, 128), BF16),
            vmem((2, TAPS, 128), BF16),
            vmem((2, TAPS, QC), BF16),
            vmem((C, C), BF16),
            vmem((C, C), BF16),
            vmem((C, C), BF16),
            vmem((C, C), BF16),
            vmem((4, QC, 128), BF16),
            vmem((2, 512, 256), BF16),
            vmem((2, 4, 8, C), F32),
            vmem((7, 1, C), F32),
            vmem((8, C), F32),
            vmem((320, 1280), BF16),
            vmem((1280, C), BF16),
            vmem((C, C), BF16),
            vmem((C, C), BF16),
            vmem((1, 320), F32),
            vmem((POS, C), BF16),
            pltpu.SemaphoreType.DMA((20,)),
            pltpu.SemaphoreType.DMA((110,)),
            pltpu.SemaphoreType.DMA((110,)),
        ],
        compiler_params=pltpu.CompilerParams(
            collective_id=0, has_side_effects=True, vmem_limit_bytes=60 * 1024 * 1024
        ),
        name="block",
    )(
        timestep,
        freq,
        features.reshape(POS, C),
        conv1_weight.reshape(TAPS, QC),
        conv2_weight.reshape(TAPS, QC),
        conv1_bias,
        conv2_bias,
        norm1_gain,
        norm1_shift,
        norm2_gain,
        norm2_shift,
        time_weight[0],
        emb_weight[0],
        zero_weight,
        zero_bias[None],
    )
    return result.reshape(1, 1, HR, W, C)


def solution(mesh):
    placed = (
        P("batch"),
        P("batch", "branch", "rows", None, None),
        P("branch", None, None, None, "rows"),
        P("branch", None),
        P("branch", None, None, None, "rows"),
        P("branch", None),
        P("branch", None),
        P("branch", None),
        P("branch", None),
        P("branch", None),
        P("branch", None, None),
        P("branch", None, None),
        P(),
        P(),
    )
    return jax.shard_map(
        body,
        mesh=mesh,
        in_specs=placed,
        out_specs=P("batch", "branch", "rows", None, None),
        check_vma=False,
    )
```

```python
import functools
import math

import numpy as np

import jax
import jax.numpy as jnp
from jax import lax
from jax.experimental import pallas as pl
from jax.experimental.pallas import tpu as pltpu
from jax.sharding import PartitionSpec as P

C = 640
GROUP = 20
W = 64
HR = 8
POS = HR * W
QC = 160
COUNT = 2048 * GROUP
CTL = 140
MESH = pl.DeviceIdType.MESH
F32 = jnp.float32
BF16 = jnp.bfloat16


ORDER = (
    ("own", 0, "N1", "P", 0),
    ("own", 0, "N2", "P", 0),
    ("own", 0, "N1", "P", 1),
    ("own", 0, "N2", "P", 1),
    ("own", 0, "N1", "P", 2),
    ("own", 0, "N2", "P", 2),
    ("stats",),
    ("time",),
    ("piece", 0, "N1", 0),
    ("piece", 0, "N2", 0),
    ("piece", 0, "N1", 1),
    ("piece", 0, "N2", 1),
    ("edges",),
    ("piece", 0, "N1", 2),
    ("piece", 0, "N2", 2),
    ("own", 0, "N1", "C", 0),
    ("own", 0, "N2", "C", 0),
    ("own", 0, "N1", "C", 1),
    ("own", 0, "N2", "C", 1),
    ("own", 0, "N1", "C", 2),
    ("own", 0, "N2", "C", 2),
    ("own", 1, "N1", "P", 0),
    ("own", 1, "N2", "P", 0),
    ("piece", 0, "F", 0),
    ("piece", 0, "F", 1),
    ("piece", 0, "F", 2),
    ("first",),
    ("c", 0, "N1", 0),
    ("c", 0, "N2", 0),
    ("zlate0",),
    ("block", 0, "N1", 0),
    ("block", 0, "N2", 0),
    ("c", 0, "N1", 1),
    ("block", 0, "N1", 1),
    ("c", 0, "N2", 1),
    ("block", 0, "N2", 1),
    ("conv", 0, "N1", 0),
    ("c", 0, "N1", 2),
    ("c", 0, "N2", 2),
    ("block", 0, "N1", 2),
    ("block", 0, "N2", 2),
    ("own", 1, "N1", "P", 2),
    ("own", 1, "N2", "P", 1),
    ("conv", 0, "N1", 1),
    ("piece", 1, "N1", 0),
    ("conv", 0, "N2", 0),
    ("piece", 1, "N2", 0),
    ("conv", 0, "N1", 2),
    ("block", 0, "F", 0),
    ("block", 0, "F", 1),
    ("hidden", "N1"),
    ("conv", 0, "N2", 1),
    ("block", 0, "F", 2),
    ("own", 1, "N1", "P", 1),
    ("own", 1, "N2", "P", 2),
    ("own", 1, "N1", "C", 0),
    ("own", 1, "N2", "C", 1),
    ("piece", 1, "N2", 1),
    ("conv", 0, "N2", 2),
    ("hidden", "N2"),
    ("piece", 1, "N1", 2),
    ("conv", 0, "F", 0),
    ("piece", 1, "F", 0),
    ("conv", 0, "F", 1),
    ("conv", 0, "F", 2),
    ("hidden", "F"),
    ("piece", 1, "N1", 1),
    ("own", 1, "N1", "C", 1),
    ("own", 1, "N2", "C", 0),
    ("own", 1, "N1", "C", 2),
    ("own", 1, "N2", "C", 2),
    ("piece", 1, "N2", 2),
    ("c", 1, "N1", 0),
    ("block", 1, "N1", 0),
    ("c", 1, "N2", 1),
    ("block", 1, "N2", 1),
    ("second",),
    ("c", 1, "N1", 1),
    ("piece", 1, "F", 1),
    ("block", 1, "N1", 1),
    ("conv", 1, "N1", 0),
    ("c", 1, "N1", 2),
    ("block", 1, "N1", 2),
    ("c", 1, "N2", 0),
    ("block", 1, "N2", 0),
    ("conv", 1, "N1", 1),
    ("c", 1, "N2", 2),
    ("piece", 1, "F", 2),
    ("block", 1, "N2", 2),
    ("conv", 1, "N1", 2),
    ("conv", 1, "N2", 0),
    ("block", 1, "F", 0),
    ("conv", 1, "N2", 1),
    ("conv", 1, "N2", 2),
    ("block", 1, "F", 1),
    ("conv", 1, "F", 0),
    ("conv", 1, "F", 1),
    ("block", 1, "F", 2),
    ("conv", 1, "F", 2),
)
AHEAD = {
    (0, "N1", 2),
    (0, "N2", 2),
    (0, "F", 1),
    (0, "F", 2),
    (1, "N1", 0),
    (1, "N1", 1),
    (1, "N1", 2),
    (1, "N2", 0),
    (1, "N2", 1),
    (1, "N2", 2),
}


def group_of(c):
    return (c * 3277) >> 16


def iota(shape, dim):
    return lax.broadcasted_iota(jnp.int32, shape, dim)


def split3(x):
    hi = x.astype(BF16).astype(F32)
    left = x - hi
    mid = left.astype(BF16).astype(F32)
    return jnp.concatenate([hi, mid, left - mid], axis=0).astype(BF16)


def exact_dot(x, m):
    out = jnp.dot(split3(x), m, preferred_element_type=F32)
    return out[0:8] + out[8:16] + out[16:24]


def silu(x):
    h = 0.5 * x
    return h + h * jnp.tanh(h)


class Links:
    def __init__(self, send, recv):
        self.send, self.recv = send, recv
        self.keys, self.started, self.count = {}, [], 0

    def slot(self, key):
        return self.keys.setdefault(key, len(self.keys))

    def prepare(self, key, src, dst, device):
        copy = pltpu.make_async_remote_copy(
            src_ref=src,
            dst_ref=dst,
            send_sem=self.send.at[self.count],
            recv_sem=self.recv.at[self.slot(key)],
            device_id=device,
            device_id_type=MESH,
        )
        self.count += 1
        self.started.append(copy)
        return copy

    def put(self, key, src, dst, device):
        self.prepare(key, src, dst, device).start()

    def get(self, key, dst, device):
        pltpu.make_async_remote_copy(
            src_ref=dst,
            dst_ref=dst,
            send_sem=self.send.at[0],
            recv_sem=self.recv.at[self.slot(key)],
            device_id=device,
            device_id_type=MESH,
        ).wait_recv()

    def drain(self):
        for copy in self.started:
            copy.wait_send()


def kernel(
    ts, freq, feats, w1, w2, b1, b2, g1, s1, g2, s2, tw, ew, zw, zb,
    outv,
    src, hid, xcat, acc, ctl, wt, group, stats, sums2, vin, shift, bias2, res, twv, ewv, zwv, fr,
    lsem, send, recv,
):
    x = lax.axis_index("rows")
    b = lax.axis_index("batch")
    branch = lax.axis_index("branch")
    core = b % 2
    zh = (b // 2) % 4
    y = b // 8
    label = (y + 2 * zh) % 4

    def along_x(by):
        return {"rows": (x + by) % 4}

    def along_batch(ny, nz, nc):
        return {"batch": (ny * 4 + nz) * 2 + nc}

    right, left, across = along_x(1), along_x(3), along_x(2)
    n1q = x + 1 - 2 * (x % 2)
    n2q = 3 - x
    n1, n2 = {"rows": n1q}, {"rows": n2q}
    up, down = along_batch((y + 1) % 4, zh, core), along_batch((y + 3) % 4, zh, core)
    front, back = along_batch(y, (zh + 1) % 4, core), along_batch(y, (zh + 3) % 4, core)
    twin = along_batch(y, zh, 1 - core)
    mate = {"branch": 1 - branch}

    barrier = pltpu.get_barrier_semaphore()
    for device in (right, left, across, up, down, front, back, twin, mate):
        pl.semaphore_signal(barrier, inc=1, device_id=device, device_id_type=MESH)

    local = {}

    def load(name, a, to):
        copy = pltpu.make_async_copy(a, to, lsem.at[len(local)])
        copy.start()
        local[name] = copy

    weights = (w1, w2)
    for t in range(5):
        load(f"feats{t}", feats.at[:, pl.ds(128 * t, 128)], src.at[t, pl.ds(W, POS), :])
    own_rows = pl.ds(pl.multiple_of(QC * x, 32), QC)
    load("fr", freq, fr)
    for i, ref in enumerate((b1, b2, g1, s1, g2, s2)):
        load(f"vec{i}", ref, vin.at[i])
    load("vec6", zb, vin.at[6, 0])

    pl.semaphore_wait(barrier, 9)
    net = Links(send, recv)
    put, get = net.put, net.get

    quarter = {"own": x, "N1": n1q, "N2": n2q, "F": (x + 2) % 4}
    side = {"N1": n1, "N2": n2}

    def piece(v, rel, u, d):
        row = pl.multiple_of(QC * quarter[rel] + 80 * core + 16 * u, 16)
        return wt.at[v, pl.ds(3 * d, 3), pl.ds(row, 16), :]

    def block(v, rel, c, d):
        row = pl.multiple_of(QC * quarter[rel] + 80 * c, 16)
        return wt.at[v, pl.ds(3 * d, 3), pl.ds(row, 80), :]

    def send_own(v, rel, kind, d):
        u = label if kind == "P" else 4
        a = weights[v].at[pl.ds(3 * d, 3), pl.ds(pl.multiple_of(80 * core + 16 * u, 16), 16), :]
        put((v, rel, kind, d), a, piece(v, "own", u, d), side[rel])

    def z_put(v, rel, d):
        ref = piece(v, rel, label, d)
        ahead = jnp.where((branch == 1) & (v == 1), 3, 1 if (v, rel, d) in AHEAD else 3)
        return net.prepare((v, rel, "Z", d), ref, ref, along_batch(y, (zh + ahead) % 4, core))

    late, passed = ([], []), [False, True]

    def on_piece(v, rel, d):
        ref = piece(v, rel, label, d)
        came = rel if rel != "F" else ("N1" if d < 2 else "N2")
        get((v, rel, "P", d), ref, side["N2" if came == "N1" else "N1"] if rel == "F" else side[rel])
        if rel == "N1" and d < 2:
            put((v, "F", "P", d), ref, ref, n2)
        if rel == "N2" and d == 2:
            put((v, "F", "P", d), ref, ref, n1)
        put((v, rel, "Yd", d), ref, ref, up)
        put((v, rel, "Yu", d), ref, ref, down)
        copy = z_put(v, rel, d)
        if passed[v]:
            copy.start()
        else:
            pl.when(branch == 0)(copy.start)
            late[v].append(copy)

    def z_late(v):
        passed[v] = True

        @pl.when(branch == 1)
        def _():
            for copy in late[v]:
                copy.start()

    def on_c(v, rel, d):
        ref = piece(v, rel, 4, d)
        get((v, rel, "C", d), ref, side[rel])
        if rel == "N1" and d == 0:
            put((v, "F", "C", d), ref, ref, n2)
        if rel == "N2" and d > 0:
            put((v, "F", "C", d), ref, ref, n1)

    def on_block(v, rel, d):
        if rel == "F":
            get((v, "F", "C", d), piece(v, "F", 4, d), n2 if d == 0 else n1)
        get((v, rel, "Yu", d), piece(v, rel, (label + 1) % 4, d), up)
        get((v, rel, "Yd", d), piece(v, rel, (label + 3) % 4, d), down)
        get((v, rel, "Z", d), piece(v, rel, (label + 2) % 4, d), back if (v, rel, d) in AHEAD else front)
        ref = block(v, rel, core, d)
        put((v, rel, "S", d), ref, ref, twin)

    def twin_block(v, rel, d):
        get((v, rel, "S", d), block(v, rel, 1 - core, d), twin)

    count = {"N1": 2, "N2": 1, "F": 2}

    def tile(rel, at):
        if rel == "N1":
            return jnp.where(at < 2, 0, 3)
        if rel == "N2":
            return jnp.where(at == 0, 4, jnp.where(at == 3, 0, 2))
        return (at + 2) % 4

    def tiles(rel, at):
        return pl.ds(tile(rel, at), count[rel])

    def group_matrix():
        for k in range(10):
            i = iota((64, C), 0) + 64 * k
            j = iota((64, C), 1)
            group[pl.ds(64 * k, 64), :] = jnp.where(group_of(i) == group_of(j), 1.0, 0.0).astype(BF16)

    def in_rows(total, square):
        row = iota((8, total.shape[1]), 0)
        return jnp.where(
            row == 0,
            jnp.sum(total, axis=0, keepdims=True),
            jnp.where(row == 1, jnp.sum(square, axis=0, keepdims=True), 0.0),
        )

    def moments(total):
        both = exact_dot(total, group[...]) * (1.0 / COUNT)
        mean = both[0:1]
        var = both[1:2] - mean * mean
        return mean, lax.rsqrt(var + 1e-05)

    def halo(buf, t, key):
        put((key, "top"), buf.at[t(x), pl.ds(POS, W), :], buf.at[t(x), pl.ds(0, W), :], right)
        put((key, "end"), buf.at[t(x), pl.ds(W, W), :], buf.at[t(x), pl.ds(POS + W, W), :], left)

    def wait_halo(buf, t, key):
        get((key, "top"), buf.at[t((x + 3) % 4), pl.ds(0, W), :], left)
        get((key, "end"), buf.at[t((x + 1) % 4), pl.ds(POS + W, W), :], right)

    def all_tiles(at):
        return pl.ds(0, 5)

    def activate(buf, mean, scale, shift):
        def step(i, _):
            rows = pl.ds(pl.multiple_of(W * i, W), W)
            outside = ((i == 0) & (x == 0)) | ((i == 9) & (x == 3))
            keep = jnp.where(outside, 0.0, 1.0)
            col = iota((W, 128), 0)
            for t in range(5):
                lanes = slice(128 * t, 128 * t + 128)
                v = buf[t, rows, :].astype(F32)
                a = silu((v - mean[:, lanes]) * scale[:, lanes] + shift[:, lanes]) * keep
                first = jnp.where(col == 0, 0.0, pltpu.roll(a, 1, 0))
                last = jnp.where(col == W - 1, 0.0, pltpu.roll(a, W - 1, 0))
                for k, part in enumerate((first, a, last)):
                    xcat[rows, pl.ds(C * k + 128 * t, 128)] = part.astype(BF16)
            return 0

        lax.fori_loop(0, 10, step, 0)

    def conv(v, t, n, d):
        rows = pl.ds(pl.multiple_of(128 * t, 128), 128 * n)
        rhs = jnp.concatenate([wt[v, 3 * d + k, rows, :] for k in range(3)], axis=1)
        for i in range(2):
            half = pl.ds(POS // 2 * i, POS // 2)
            lhs = xcat[pl.ds(W * d + POS // 2 * i, POS // 2), :]
            r = lax.dot_general(lhs, rhs, (((1,), (1,)), ((), ())), preferred_element_type=F32)
            for k in range(n):
                part = r[:, 128 * k : 128 * k + 128]
                acc[t + k, half, :] = part if d == 0 else acc[t + k, half, :] + part

    def add_up(values):
        total, square = 0.0, 0.0
        for k in range(values.shape[0] // 8):
            part = values[8 * k : 8 * k + 8]
            total, square = total + part, square + part * part
        return total, square

    def do_edges():
        halo(src, all_tiles, "features")

    def do_stats():
        load("tw", tw, twv)
        load("ew", ew, ewv)
        load("own0", w1, wt.at[0, :, own_rows, :])
        for t in range(5):
            local[f"feats{t}"].wait()

        def step(i, carry):
            rows = pl.ds(pl.multiple_of(W + W * i, W), W)
            new = []
            for t in range(5):
                total, square = add_up(src[t, rows, :].astype(F32))
                new += [carry[2 * t] + total, carry[2 * t + 1] + square]
            return tuple(new)

        carry = lax.fori_loop(0, HR, step, (jnp.zeros((8, 128), F32),) * 10)
        stats[x] = in_rows(jnp.concatenate(carry[0::2], axis=1), jnp.concatenate(carry[1::2], axis=1))
        group_matrix()
        for by, device in ((1, right), (2, across), (3, left)):
            put(("stats", by), stats.at[x], stats.at[x], device)
        load("own1", w2, wt.at[1, :, own_rows, :])
        load("zw", zw, zwv)

    def do_time():
        for i in range(7):
            local[f"vec{i}"].wait()
        local["fr"].wait()
        local["tw"].wait()
        local["ew"].wait()
        angle = jnp.broadcast_to(fr[...] * ts[0].astype(F32), (8, 320))
        n = jnp.floor(angle * (2.0 / math.pi) + 0.5)
        r = ((angle - n * 1.5703125) - n * 4.837512969970703e-4) - n * 7.549790126404332e-8
        turn = n + jnp.where(iota((8, 320), 1) < 160, 1.0, 0.0)
        turn = turn - 4.0 * jnp.floor(turn * 0.25)
        r2 = r * r
        sin_r = r + r * r2 * (-1.0 / 6 + r2 * (1.0 / 120 + r2 * (-1.0 / 5040 + r2 * (1.0 / 362880))))
        cos_r = 1.0 + r2 * (-0.5 + r2 * (1.0 / 24 + r2 * (-1.0 / 720 + r2 * (1.0 / 40320 - r2 * (1.0 / 3628800)))))
        waves = jnp.where(
            turn < 0.5, sin_r, jnp.where(turn < 1.5, cos_r, jnp.where(turn < 2.5, -sin_r, -cos_r))
        )
        inner = silu(exact_dot(waves, twv[...]))
        extra = vin[0] + exact_dot(inner, ewv[...])
        for t in range(5):
            shift[t] = extra[:, 128 * t : 128 * t + 128]
            bias2[t] = jnp.broadcast_to(vin[1][:, 128 * t : 128 * t + 128], (8, 128))

    def do_first():
        wait_halo(src, all_tiles, "features")
        for by, device in ((1, left), (2, across), (3, right)):
            get(("stats", by), stats.at[(x - by + 4) % 4], device)
        mean, scale = moments(stats[0] + stats[1] + stats[2] + stats[3])
        activate(src, mean, scale * vin[2], vin[3])

    def do_hidden(rel):
        for k in range(count[rel]):
            t = tile(rel, x) + k

            def step(i, carry):
                rows = pl.ds(pl.multiple_of(W * i, W), W)
                h = (acc[t, rows, :] + shift[t][0:1]).astype(BF16)
                hid[t, pl.ds(pl.multiple_of(W + W * i, W), W), :] = h
                total, square = add_up(h.astype(F32))
                return carry[0] + total, carry[1] + square

            zero = jnp.zeros((8, 128), F32)
            total, square = lax.fori_loop(0, HR, step, (zero, zero))
            sums2[x, t] = in_rows(total, square)
        halo(hid, lambda at: tiles(rel, at), ("hidden", rel))
        ref = sums2.at[x, tiles(rel, x)]
        for by, device in ((1, right), (2, across), (3, left)):
            put(("sums", rel, by), ref, ref, device)

    def do_second():
        for rel in ("N1", "N2", "F"):
            wait_halo(hid, lambda at: tiles(rel, at), ("hidden", rel))
            for by, device in ((1, left), (2, across), (3, right)):
                at = (x - by + 4) % 4
                get(("sums", rel, by), sums2.at[at, tiles(rel, at)], device)
        total = [sums2[0, t] + sums2[1, t] + sums2[2, t] + sums2[3, t] for t in range(5)]
        mean, scale = moments(jnp.concatenate(total, axis=1))
        activate(hid, mean, scale * vin[4], vin[5])

    slots = {"N1": 0, "N2": 2, "F": 3}

    def ctl_copy(rel, k):
        t = tile(rel, x) + k
        slot = CTL + slots[rel] + k
        return pltpu.make_async_remote_copy(
            src_ref=ctl.at[t],
            dst_ref=ctl.at[t],
            send_sem=send.at[slot],
            recv_sem=recv.at[slot],
            device_id=mate,
            device_id_type=MESH,
        )

    def pre(t, rows):
        own = src[t, pl.ds(W + rows.start, rows.size), :].astype(F32)
        return own + acc[t, rows, :] + bias2[t][0:1]

    def give(rel):
        @pl.when(branch == 0)
        def _():
            for k in range(count[rel]):
                t = tile(rel, x) + k
                ctl[t] = pre(t, pl.ds(0, POS)).astype(BF16)
                ctl_copy(rel, k).start()

    def do_conv(v, rel, d):
        if rel == "N1" and d == 0:
            local[f"own{v}"].wait()
        twin_block(v, rel, d)
        conv(v, tile(rel, x), count[rel], d)
        if v == 1 and d == 2:
            give(rel)

    steps = {
        "own": send_own,
        "piece": on_piece,
        "c": on_c,
        "block": on_block,
        "conv": do_conv,
        "zlate0": lambda: z_late(0),
        "edges": do_edges,
        "stats": do_stats,
        "time": do_time,
        "first": do_first,
        "hidden": do_hidden,
        "second": do_second,
    }
    for step in ORDER:
        steps[step[0]](*step[1:])
    local["zw"].wait()

    @pl.when(branch == 1)
    def _():
        for rel in ("N1", "N2", "F"):
            n = count[rel]
            t = tile(rel, x)
            for k in range(n):
                ctl_copy(rel, k).wait_recv()

            def step(i, _):
                rows = pl.ds(pl.multiple_of(128 * i, 128), 128)
                lhs = jnp.concatenate([ctl[t + k, rows, :] for k in range(n)], axis=1)
                rhs = zwv[pl.ds(pl.multiple_of(128 * t, 128), 128 * n), :]
                r = jnp.dot(lhs, rhs, preferred_element_type=F32)
                if rel == "N1":
                    res[rows, :] = r + vin[6]
                elif rel == "N2":
                    res[rows, :] = res[rows, :] + r
                else:
                    r = (res[rows, :] + r).astype(BF16).astype(F32)
                    for k in range(5):
                        lanes = slice(128 * k, 128 * k + 128)
                        outv[rows, pl.ds(128 * k, 128)] = (pre(k, rows) + r[:, lanes]).astype(BF16)
                return 0

            lax.fori_loop(0, 4, step, 0)

    @pl.when(branch == 0)
    def _():
        for t in range(5):
            outv[:, pl.ds(128 * t, 128)] = ctl[t]
        for rel in ("N1", "N2", "F"):
            for k in range(count[rel]):
                ctl_copy(rel, k).wait_send()

    net.drain()


def body(
    timestep,
    features,
    conv1_weight,
    conv1_bias,
    conv2_weight,
    conv2_bias,
    norm1_gain,
    norm1_shift,
    norm2_gain,
    norm2_shift,
    time_weight,
    emb_weight,
    zero_weight,
    zero_bias,
):
    half = 160
    line = np.exp(-math.log(10000.0) * np.arange(half, dtype=np.float32) / np.float32(half))
    freq = jnp.asarray(np.concatenate([line, line])[None].astype(np.float32))
    hbm = pl.BlockSpec(memory_space=pltpu.HBM)
    vmem = pltpu.VMEM
    result = pl.pallas_call(
        kernel,
        out_shape=pltpu.VMEM((POS, C), BF16),
        in_specs=[pl.BlockSpec(memory_space=pltpu.SMEM)] + [hbm] * 14,
        out_specs=pl.BlockSpec(memory_space=pltpu.VMEM),
        scratch_shapes=[
            vmem((5, POS + 2 * W, 128), BF16),
            vmem((5, POS + 2 * W, 128), BF16),
            vmem((POS + 2 * W, 3 * C), BF16),
            vmem((5, POS, 128), F32),
            vmem((5, POS, 128), BF16),
            vmem((2, 9, C, C), BF16),
            vmem((C, C), BF16),
            vmem((4, 8, C), F32),
            vmem((4, 5, 8, 128), F32),
            vmem((7, 1, C), F32),
            vmem((5, 8, 128), F32),
            vmem((5, 8, 128), F32),
            vmem((POS, C), F32),
            vmem((320, 1280), BF16),
            vmem((1280, C), BF16),
            vmem((C, C), BF16),
            vmem((1, 320), F32),
            pltpu.SemaphoreType.DMA((20,)),
            pltpu.SemaphoreType.DMA((CTL + 5,)),
            pltpu.SemaphoreType.DMA((CTL + 5,)),
        ],
        compiler_params=pltpu.CompilerParams(
            collective_id=0, has_side_effects=True, vmem_limit_bytes=60 * 1024 * 1024
        ),
        name="block",
    )(
        timestep,
        freq,
        features.reshape(POS, C),
        jnp.swapaxes(conv1_weight, 3, 4).reshape(9, QC, C),
        jnp.swapaxes(conv2_weight, 3, 4).reshape(9, QC, C),
        conv1_bias,
        conv2_bias,
        norm1_gain,
        norm1_shift,
        norm2_gain,
        norm2_shift,
        time_weight[0],
        emb_weight[0],
        zero_weight,
        zero_bias,
    )
    return result.reshape(1, 1, HR, W, C)


def solution(mesh):
    placed = (
        P("batch"),
        P("batch", "branch", "rows", None, None),
        P("branch", None, None, None, "rows"),
        P("branch", None),
        P("branch", None, None, None, "rows"),
        P("branch", None),
        P("branch", None),
        P("branch", None),
        P("branch", None),
        P("branch", None),
        P("branch", None, None),
        P("branch", None, None),
        P(),
        P(),
    )
    return jax.shard_map(
        body,
        mesh=mesh,
        in_specs=placed,
        out_specs=P("batch", "branch", "rows", None, None),
        check_vma=False,
    )
```

```python
import functools
import math

import numpy as np

import jax
import jax.numpy as jnp
from jax import lax
from jax.experimental import pallas as pl
from jax.experimental.pallas import tpu as pltpu
from jax.sharding import PartitionSpec as P

C = 640
GROUP = 20
W = 64
HR = 8
POS = HR * W
QC = 160
COUNT = 2048 * GROUP
CTL = 140
MESH = pl.DeviceIdType.MESH
F32 = jnp.float32
BF16 = jnp.bfloat16


OWN = "own"
PIECE = "piece"
REST = "c"
BLOCK = "block"
CONV = "conv"
FORWARD = "fwd"
LATE = "zlate0"
EDGES = "edges"
STATS = "stats"
TIME = "time"
FIRST = "first"
HIDDEN = "hidden"
SECOND = "second"
N1 = "N1"
N2 = "N2"
FAR = "F"
MAIN = "P"
LAST = "C"
ORDER = (
    (OWN, 0, N1, MAIN, 1),
    (OWN, 0, N2, MAIN, 2),
    (OWN, 0, N1, MAIN, 2),
    (OWN, 0, N2, MAIN, 0),
    (OWN, 0, N2, LAST, 0),
    (OWN, 0, N1, MAIN, 0),
    (OWN, 0, N1, LAST, 2),
    (OWN, 0, N2, MAIN, 1),
    (STATS,),
    (OWN, 0, N1, LAST, 0),
    (OWN, 0, N2, LAST, 2),
    (TIME,),
    (OWN, 0, N2, LAST, 1),
    (PIECE, 0, N2, 2),
    (PIECE, 0, N1, 2),
    (PIECE, 0, N1, 0),
    (OWN, 0, N1, LAST, 1),
    (OWN, 1, N1, MAIN, 0),
    (PIECE, 0, N2, 1),
    (REST, 0, N1, 2),
    (PIECE, 0, N1, 1),
    (EDGES,),
    (OWN, 1, N2, MAIN, 2),
    (PIECE, 0, N2, 0),
    (OWN, 1, N1, MAIN, 1),
    (LATE,),
    (BLOCK, 0, N1, 2),
    (PIECE, 0, FAR, 0),
    (REST, 0, N1, 0),
    (OWN, 1, N1, MAIN, 2),
    (REST, 0, N2, 1),
    (PIECE, 0, FAR, 1),
    (PIECE, 0, FAR, 2),
    (OWN, 1, N2, MAIN, 0),
    (BLOCK, 0, N1, 0),
    (BLOCK, 0, N2, 1),
    (REST, 0, N1, 1),
    (OWN, 1, N2, MAIN, 1),
    (REST, 0, N2, 2),
    (REST, 0, N2, 0),
    (BLOCK, 0, N1, 1),
    (OWN, 1, N2, LAST, 2),
    (PIECE, 1, N1, 0),
    (FIRST,),
    (BLOCK, 0, N2, 0),
    (OWN, 1, N1, LAST, 2),
    (CONV, 0, N1, 0),
    (OWN, 1, N2, LAST, 1),
    (PIECE, 1, N2, 2),
    (OWN, 1, N2, LAST, 0),
    (BLOCK, 0, N2, 2),
    (CONV, 0, N1, 1),
    (OWN, 1, N1, LAST, 0),
    (OWN, 1, N1, LAST, 1),
    (CONV, 0, N1, 2),
    (BLOCK, 0, FAR, 0),
    (CONV, 0, N2, 0),
    (PIECE, 1, N1, 2),
    (PIECE, 1, N1, 1),
    (HIDDEN, N1),
    (FORWARD, N2, 2),
    (BLOCK, 0, FAR, 1),
    (FORWARD, N1, 0),
    (CONV, 0, N2, 1),
    (BLOCK, 0, FAR, 2),
    (CONV, 0, N2, 2),
    (CONV, 0, FAR, 0),
    (PIECE, 1, N2, 0),
    (HIDDEN, N2),
    (CONV, 0, FAR, 1),
    (CONV, 0, FAR, 2),
    (HIDDEN, FAR),
    (PIECE, 1, N2, 1),
    (REST, 1, N2, 1),
    (FORWARD, N1, 1),
    (REST, 1, N1, 0),
    (BLOCK, 1, N1, 0),
    (PIECE, 1, FAR, 0),
    (REST, 1, N2, 2),
    (REST, 1, N1, 2),
    (REST, 1, N2, 0),
    (REST, 1, N1, 1),
    (BLOCK, 1, N1, 1),
    (PIECE, 1, FAR, 2),
    (BLOCK, 1, N1, 2),
    (BLOCK, 1, N2, 0),
    (SECOND,),
    (PIECE, 1, FAR, 1),
    (BLOCK, 1, N2, 1),
    (CONV, 1, N1, 0),
    (CONV, 1, N1, 1),
    (CONV, 1, N1, 2),
    (BLOCK, 1, FAR, 0),
    (BLOCK, 1, FAR, 2),
    (CONV, 1, N2, 0),
    (BLOCK, 1, N2, 2),
    (CONV, 1, N2, 1),
    (BLOCK, 1, FAR, 1),
    (CONV, 1, FAR, 0),
    (CONV, 1, N2, 2),
    (CONV, 1, FAR, 1),
    (CONV, 1, FAR, 2),
)
AHEAD = {
    (0, FAR, 2),
    (0, N1, 2),
    (0, N2, 1),
    (1, FAR, 0),
    (1, FAR, 1),
    (1, FAR, 2),
    (1, N1, 0),
    (1, N1, 1),
    (1, N1, 2),
    (1, N2, 0),
    (1, N2, 1),
    (1, N2, 2),
}


def group_of(c):
    return (c * 3277) >> 16


def iota(shape, dim):
    return lax.broadcasted_iota(jnp.int32, shape, dim)


def split3(x):
    hi = x.astype(BF16).astype(F32)
    left = x - hi
    mid = left.astype(BF16).astype(F32)
    return jnp.concatenate([hi, mid, left - mid], axis=0).astype(BF16)


def exact_dot(x, m):
    out = jnp.dot(split3(x), m, preferred_element_type=F32)
    return out[0:8] + out[8:16] + out[16:24]


def silu(x):
    h = 0.5 * x
    return h + h * jnp.tanh(h)


class Links:
    def __init__(self, send, recv):
        self.send, self.recv = send, recv
        self.keys, self.started, self.count = {}, [], 0

    def slot(self, key):
        return self.keys.setdefault(key, len(self.keys))

    def prepare(self, key, src, dst, device):
        copy = pltpu.make_async_remote_copy(
            src_ref=src,
            dst_ref=dst,
            send_sem=self.send.at[self.count],
            recv_sem=self.recv.at[self.slot(key)],
            device_id=device,
            device_id_type=MESH,
        )
        self.count += 1
        self.started.append(copy)
        return copy

    def put(self, key, src, dst, device):
        self.prepare(key, src, dst, device).start()

    def get(self, key, dst, device):
        pltpu.make_async_remote_copy(
            src_ref=dst,
            dst_ref=dst,
            send_sem=self.send.at[0],
            recv_sem=self.recv.at[self.slot(key)],
            device_id=device,
            device_id_type=MESH,
        ).wait_recv()

    def drain(self):
        for copy in self.started:
            copy.wait_send()


def kernel(
    ts, freq, feats, w1, w2, b1, b2, g1, s1, g2, s2, tw, ew, zw, zb,
    outv,
    src, hid, xcat, acc, ctl, wt, group, stats, sums2, vin, shift, bias2, res, twv, ewv, zwv, fr,
    lsem, send, recv,
):
    x = lax.axis_index("rows")
    b = lax.axis_index("batch")
    branch = lax.axis_index("branch")
    core = b % 2
    zh = (b // 2) % 4
    y = b // 8
    label = (y + 2 * zh) % 4

    def along_x(by):
        return {"rows": (x + by) % 4}

    def along_batch(ny, nz, nc):
        return {"batch": (ny * 4 + nz) * 2 + nc}

    right, left, across = along_x(1), along_x(3), along_x(2)
    n1q = x + 1 - 2 * (x % 2)
    n2q = 3 - x
    n1, n2 = {"rows": n1q}, {"rows": n2q}
    up, down = along_batch((y + 1) % 4, zh, core), along_batch((y + 3) % 4, zh, core)
    front, back = along_batch(y, (zh + 1) % 4, core), along_batch(y, (zh + 3) % 4, core)
    twin = along_batch(y, zh, 1 - core)
    mate = {"branch": 1 - branch}

    barrier = pltpu.get_barrier_semaphore()
    for device in (right, left, across, up, down, front, back, twin, mate):
        pl.semaphore_signal(barrier, inc=1, device_id=device, device_id_type=MESH)

    local = {}

    def load(name, a, to):
        copy = pltpu.make_async_copy(a, to, lsem.at[len(local)])
        copy.start()
        local[name] = copy

    weights = (w1, w2)
    for t in range(5):
        load(f"feats{t}", feats.at[:, pl.ds(128 * t, 128)], src.at[t, pl.ds(W, POS), :])
    own_rows = pl.ds(pl.multiple_of(QC * x, 32), QC)
    load("fr", freq, fr)
    for i, ref in enumerate((b1, b2, g1, s1, g2, s2)):
        load(f"vec{i}", ref, vin.at[i])
    load("vec6", zb, vin.at[6, 0])

    pl.semaphore_wait(barrier, 9)
    net = Links(send, recv)
    put, get = net.put, net.get

    quarter = {"own": x, "N1": n1q, "N2": n2q, "F": (x + 2) % 4}
    side = {"N1": n1, "N2": n2}

    def piece(v, rel, u, d):
        row = pl.multiple_of(QC * quarter[rel] + 80 * core + 16 * u, 16)
        return wt.at[v, pl.ds(3 * d, 3), pl.ds(row, 16), :]

    def block(v, rel, c, d):
        row = pl.multiple_of(QC * quarter[rel] + 80 * c, 16)
        return wt.at[v, pl.ds(3 * d, 3), pl.ds(row, 80), :]

    def send_own(v, rel, kind, d):
        u = label if kind == "P" else 4
        a = weights[v].at[pl.ds(3 * d, 3), pl.ds(pl.multiple_of(80 * core + 16 * u, 16), 16), :]
        put((v, rel, kind, d), a, piece(v, "own", u, d), side[rel])

    def z_put(v, rel, d):
        ref = piece(v, rel, label, d)
        ahead = jnp.where((branch == 1) & (v == 1), 3, 1 if (v, rel, d) in AHEAD else 3)
        return net.prepare((v, rel, "Z", d), ref, ref, along_batch(y, (zh + ahead) % 4, core))

    late, passed = ([], []), [False, True]

    def forward(v, rel, d):
        ref = piece(v, rel, label, d)
        if rel == "N1" and d < 2:
            put((v, "F", "P", d), ref, ref, n2)
        if rel == "N2" and d == 2:
            put((v, "F", "P", d), ref, ref, n1)

    def on_piece(v, rel, d):
        ref = piece(v, rel, label, d)
        came = rel if rel != "F" else ("N1" if d < 2 else "N2")
        get((v, rel, "P", d), ref, side["N2" if came == "N1" else "N1"] if rel == "F" else side[rel])
        if v == 0:
            forward(v, rel, d)
        put((v, rel, "Yd", d), ref, ref, up)
        put((v, rel, "Yu", d), ref, ref, down)
        copy = z_put(v, rel, d)
        if passed[v]:
            copy.start()
        else:
            pl.when(branch == 0)(copy.start)
            late[v].append(copy)

    def z_late(v):
        passed[v] = True

        @pl.when(branch == 1)
        def _():
            for copy in late[v]:
                copy.start()

    def on_c(v, rel, d):
        ref = piece(v, rel, 4, d)
        get((v, rel, "C", d), ref, side[rel])
        if rel == "N1" and d == 0:
            put((v, "F", "C", d), ref, ref, n2)
        if rel == "N2" and d > 0:
            put((v, "F", "C", d), ref, ref, n1)

    def on_block(v, rel, d):
        if rel == "F":
            get((v, "F", "C", d), piece(v, "F", 4, d), n2 if d == 0 else n1)
        get((v, rel, "Yu", d), piece(v, rel, (label + 1) % 4, d), up)
        get((v, rel, "Yd", d), piece(v, rel, (label + 3) % 4, d), down)
        get((v, rel, "Z", d), piece(v, rel, (label + 2) % 4, d), back if (v, rel, d) in AHEAD else front)
        ref = block(v, rel, core, d)
        put((v, rel, "S", d), ref, ref, twin)

    def twin_block(v, rel, d):
        get((v, rel, "S", d), block(v, rel, 1 - core, d), twin)

    count = {"N1": 2, "N2": 1, "F": 2}

    def tile(rel, at):
        if rel == "N1":
            return jnp.where(at < 2, 0, 3)
        if rel == "N2":
            return jnp.where(at == 0, 4, jnp.where(at == 3, 0, 2))
        return (at + 2) % 4

    def tiles(rel, at):
        return pl.ds(tile(rel, at), count[rel])

    def group_matrix():
        for k in range(10):
            i = iota((64, C), 0) + 64 * k
            j = iota((64, C), 1)
            group[pl.ds(64 * k, 64), :] = jnp.where(group_of(i) == group_of(j), 1.0, 0.0).astype(BF16)

    def in_rows(total, square):
        row = iota((8, total.shape[1]), 0)
        return jnp.where(
            row == 0,
            jnp.sum(total, axis=0, keepdims=True),
            jnp.where(row == 1, jnp.sum(square, axis=0, keepdims=True), 0.0),
        )

    def moments(total):
        both = exact_dot(total, group[...]) * (1.0 / COUNT)
        mean = both[0:1]
        var = both[1:2] - mean * mean
        return mean, lax.rsqrt(var + 1e-05)

    def halo(buf, t, key):
        put((key, "top"), buf.at[t(x), pl.ds(POS, W), :], buf.at[t(x), pl.ds(0, W), :], right)
        put((key, "end"), buf.at[t(x), pl.ds(W, W), :], buf.at[t(x), pl.ds(POS + W, W), :], left)

    def wait_halo(buf, t, key):
        get((key, "top"), buf.at[t((x + 3) % 4), pl.ds(0, W), :], left)
        get((key, "end"), buf.at[t((x + 1) % 4), pl.ds(POS + W, W), :], right)

    def all_tiles(at):
        return pl.ds(0, 5)

    def activate(buf, mean, scale, shift):
        def step(i, _):
            rows = pl.ds(pl.multiple_of(W * i, W), W)
            outside = ((i == 0) & (x == 0)) | ((i == 9) & (x == 3))
            keep = jnp.where(outside, 0.0, 1.0)
            col = iota((W, 128), 0)
            for t in range(5):
                lanes = slice(128 * t, 128 * t + 128)
                v = buf[t, rows, :].astype(F32)
                a = silu((v - mean[:, lanes]) * scale[:, lanes] + shift[:, lanes]) * keep
                first = jnp.where(col == 0, 0.0, pltpu.roll(a, 1, 0))
                last = jnp.where(col == W - 1, 0.0, pltpu.roll(a, W - 1, 0))
                for k, part in enumerate((first, a, last)):
                    xcat[rows, pl.ds(C * k + 128 * t, 128)] = part.astype(BF16)
            return 0

        lax.fori_loop(0, 10, step, 0)

    def conv(v, t, n, d):
        rows = pl.ds(pl.multiple_of(128 * t, 128), 128 * n)
        rhs = jnp.concatenate([wt[v, 3 * d + k, rows, :] for k in range(3)], axis=1)
        for i in range(2):
            half = pl.ds(POS // 2 * i, POS // 2)
            lhs = xcat[pl.ds(W * d + POS // 2 * i, POS // 2), :]
            r = lax.dot_general(lhs, rhs, (((1,), (1,)), ((), ())), preferred_element_type=F32)
            for k in range(n):
                part = r[:, 128 * k : 128 * k + 128]
                acc[t + k, half, :] = part if d == 0 else acc[t + k, half, :] + part

    def add_up(values):
        total, square = 0.0, 0.0
        for k in range(values.shape[0] // 8):
            part = values[8 * k : 8 * k + 8]
            total, square = total + part, square + part * part
        return total, square

    def do_edges():
        halo(src, all_tiles, "features")

    def do_stats():
        load("tw", tw, twv)
        load("ew", ew, ewv)
        load("own0", w1, wt.at[0, :, own_rows, :])
        for t in range(5):
            local[f"feats{t}"].wait()

        def step(i, carry):
            rows = pl.ds(pl.multiple_of(W + W * i, W), W)
            new = []
            for t in range(5):
                total, square = add_up(src[t, rows, :].astype(F32))
                new += [carry[2 * t] + total, carry[2 * t + 1] + square]
            return tuple(new)

        carry = lax.fori_loop(0, HR, step, (jnp.zeros((8, 128), F32),) * 10)
        stats[x] = in_rows(jnp.concatenate(carry[0::2], axis=1), jnp.concatenate(carry[1::2], axis=1))
        group_matrix()
        for by, device in ((1, right), (2, across), (3, left)):
            put(("stats", by), stats.at[x], stats.at[x], device)
        load("own1", w2, wt.at[1, :, own_rows, :])
        load("zw", zw, zwv)

    def do_time():
        for i in range(7):
            local[f"vec{i}"].wait()
        local["fr"].wait()
        local["tw"].wait()
        local["ew"].wait()
        angle = jnp.broadcast_to(fr[...] * ts[0].astype(F32), (8, 320))
        n = jnp.floor(angle * (2.0 / math.pi) + 0.5)
        r = ((angle - n * 1.5703125) - n * 4.837512969970703e-4) - n * 7.549790126404332e-8
        turn = n + jnp.where(iota((8, 320), 1) < 160, 1.0, 0.0)
        turn = turn - 4.0 * jnp.floor(turn * 0.25)
        r2 = r * r
        sin_r = r + r * r2 * (-1.0 / 6 + r2 * (1.0 / 120 + r2 * (-1.0 / 5040 + r2 * (1.0 / 362880))))
        cos_r = 1.0 + r2 * (-0.5 + r2 * (1.0 / 24 + r2 * (-1.0 / 720 + r2 * (1.0 / 40320 - r2 * (1.0 / 3628800)))))
        waves = jnp.where(
            turn < 0.5, sin_r, jnp.where(turn < 1.5, cos_r, jnp.where(turn < 2.5, -sin_r, -cos_r))
        )
        inner = silu(exact_dot(waves, twv[...]))
        extra = vin[0] + exact_dot(inner, ewv[...])
        for t in range(5):
            shift[t] = extra[:, 128 * t : 128 * t + 128]
            bias2[t] = jnp.broadcast_to(vin[1][:, 128 * t : 128 * t + 128], (8, 128))

    def do_first():
        wait_halo(src, all_tiles, "features")
        for by, device in ((1, left), (2, across), (3, right)):
            get(("stats", by), stats.at[(x - by + 4) % 4], device)
        mean, scale = moments(stats[0] + stats[1] + stats[2] + stats[3])
        activate(src, mean, scale * vin[2], vin[3])

    def do_hidden(rel):
        for k in range(count[rel]):
            t = tile(rel, x) + k

            def step(i, carry):
                rows = pl.ds(pl.multiple_of(W * i, W), W)
                h = (acc[t, rows, :] + shift[t][0:1]).astype(BF16)
                hid[t, pl.ds(pl.multiple_of(W + W * i, W), W), :] = h
                total, square = add_up(h.astype(F32))
                return carry[0] + total, carry[1] + square

            zero = jnp.zeros((8, 128), F32)
            total, square = lax.fori_loop(0, HR, step, (zero, zero))
            sums2[x, t] = in_rows(total, square)
        halo(hid, lambda at: tiles(rel, at), ("hidden", rel))
        ref = sums2.at[x, tiles(rel, x)]
        for by, device in ((1, right), (2, across), (3, left)):
            put(("sums", rel, by), ref, ref, device)

    def do_second():
        for rel in ("N1", "N2", "F"):
            wait_halo(hid, lambda at: tiles(rel, at), ("hidden", rel))
            for by, device in ((1, left), (2, across), (3, right)):
                at = (x - by + 4) % 4
                get(("sums", rel, by), sums2.at[at, tiles(rel, at)], device)
        total = [sums2[0, t] + sums2[1, t] + sums2[2, t] + sums2[3, t] for t in range(5)]
        mean, scale = moments(jnp.concatenate(total, axis=1))
        activate(hid, mean, scale * vin[4], vin[5])

    slots = {"N1": 0, "N2": 2, "F": 3}

    def ctl_copy(rel, k, half):
        t = tile(rel, x) + k
        slot = CTL + 2 * (slots[rel] + k) + half
        ref = ctl.at[t, pl.ds(POS // 2 * half, POS // 2), :]
        return pltpu.make_async_remote_copy(
            src_ref=ref,
            dst_ref=ref,
            send_sem=send.at[slot],
            recv_sem=recv.at[slot],
            device_id=mate,
            device_id_type=MESH,
        )

    def pre(t, rows):
        own = src[t, pl.ds(W + rows.start, rows.size), :].astype(F32)
        return own + acc[t, rows, :] + bias2[t][0:1]

    def give(rel):
        @pl.when(branch == 0)
        def _():
            for k in range(count[rel]):
                t = tile(rel, x) + k
                ctl[t] = pre(t, pl.ds(0, POS)).astype(BF16)
                if rel != "F":
                    for half in range(2):
                        ctl_copy(rel, k, half).start()
            if rel == "F":
                for half in range(2):
                    for k in range(2):
                        ctl_copy(rel, k, half).start()

    def do_conv(v, rel, d):
        if rel == "N1" and d == 0:
            local[f"own{v}"].wait()
        twin_block(v, rel, d)
        conv(v, tile(rel, x), count[rel], d)
        if v == 1 and d == 2:
            give(rel)

    steps = {
        "own": send_own,
        "piece": on_piece,
        "c": on_c,
        "fwd": lambda rel, d: forward(1, rel, d),
        "block": on_block,
        "conv": do_conv,
        "zlate0": lambda: z_late(0),
        "edges": do_edges,
        "stats": do_stats,
        "time": do_time,
        "first": do_first,
        "hidden": do_hidden,
        "second": do_second,
    }
    for step in ORDER:
        steps[step[0]](*step[1:])
    local["zw"].wait()

    @pl.when(branch == 1)
    def _():
        for rel in ("N1", "N2", "F"):
            n = count[rel]
            t = tile(rel, x)

            def arrive(half):
                for k in range(n):
                    ctl_copy(rel, k, half).wait_recv()

            def step(i, _):
                rows = pl.ds(pl.multiple_of(128 * i, 128), 128)
                lhs = jnp.concatenate([ctl[t + k, rows, :] for k in range(n)], axis=1)
                rhs = zwv[pl.ds(pl.multiple_of(128 * t, 128), 128 * n), :]
                r = jnp.dot(lhs, rhs, preferred_element_type=F32)
                if rel == "N1":
                    res[rows, :] = r + vin[6]
                elif rel == "N2":
                    res[rows, :] = res[rows, :] + r
                else:
                    r = (res[rows, :] + r).astype(BF16).astype(F32)
                    for k in range(5):
                        lanes = slice(128 * k, 128 * k + 128)
                        outv[rows, pl.ds(128 * k, 128)] = (pre(k, rows) + r[:, lanes]).astype(BF16)
                return 0

            for half in range(2):
                arrive(half)
                lax.fori_loop(2 * half, 2 * half + 2, step, 0)

    @pl.when(branch == 0)
    def _():
        for t in range(5):
            outv[:, pl.ds(128 * t, 128)] = ctl[t]
        for rel in ("N1", "N2", "F"):
            for k in range(count[rel]):
                for half in range(2):
                    ctl_copy(rel, k, half).wait_send()

    net.drain()


def body(
    timestep,
    features,
    conv1_weight,
    conv1_bias,
    conv2_weight,
    conv2_bias,
    norm1_gain,
    norm1_shift,
    norm2_gain,
    norm2_shift,
    time_weight,
    emb_weight,
    zero_weight,
    zero_bias,
):
    half = 160
    line = np.exp(-math.log(10000.0) * np.arange(half, dtype=np.float32) / np.float32(half))
    freq = jnp.asarray(np.concatenate([line, line])[None].astype(np.float32))
    hbm = pl.BlockSpec(memory_space=pltpu.HBM)
    vmem = pltpu.VMEM
    result = pl.pallas_call(
        kernel,
        out_shape=pltpu.VMEM((POS, C), BF16),
        in_specs=[pl.BlockSpec(memory_space=pltpu.SMEM)] + [hbm] * 14,
        out_specs=pl.BlockSpec(memory_space=pltpu.VMEM),
        scratch_shapes=[
            vmem((5, POS + 2 * W, 128), BF16),
            vmem((5, POS + 2 * W, 128), BF16),
            vmem((POS + 2 * W, 3 * C), BF16),
            vmem((5, POS, 128), F32),
            vmem((5, POS, 128), BF16),
            vmem((2, 9, C, C), BF16),
            vmem((C, C), BF16),
            vmem((4, 8, C), F32),
            vmem((4, 5, 8, 128), F32),
            vmem((7, 1, C), F32),
            vmem((5, 8, 128), F32),
            vmem((5, 8, 128), F32),
            vmem((POS, C), F32),
            vmem((320, 1280), BF16),
            vmem((1280, C), BF16),
            vmem((C, C), BF16),
            vmem((1, 320), F32),
            pltpu.SemaphoreType.DMA((20,)),
            pltpu.SemaphoreType.DMA((CTL + 10,)),
            pltpu.SemaphoreType.DMA((CTL + 10,)),
        ],
        compiler_params=pltpu.CompilerParams(
            collective_id=0, has_side_effects=True, vmem_limit_bytes=60 * 1024 * 1024
        ),
        name="block",
    )(
        timestep,
        freq,
        features.reshape(POS, C),
        jnp.swapaxes(conv1_weight, 3, 4).reshape(9, QC, C),
        jnp.swapaxes(conv2_weight, 3, 4).reshape(9, QC, C),
        conv1_bias,
        conv2_bias,
        norm1_gain,
        norm1_shift,
        norm2_gain,
        norm2_shift,
        time_weight[0],
        emb_weight[0],
        zero_weight,
        zero_bias,
    )
    return result.reshape(1, 1, HR, W, C)


def solution(mesh):
    placed = (
        P("batch"),
        P("batch", "branch", "rows", None, None),
        P("branch", None, None, None, "rows"),
        P("branch", None),
        P("branch", None, None, None, "rows"),
        P("branch", None),
        P("branch", None),
        P("branch", None),
        P("branch", None),
        P("branch", None),
        P("branch", None, None),
        P("branch", None, None),
        P(),
        P(),
    )
    return jax.shard_map(
        body,
        mesh=mesh,
        in_specs=placed,
        out_specs=P("batch", "branch", "rows", None, None),
        check_vma=False,
    )
```

```python
import functools
import math

import numpy as np

import jax
import jax.numpy as jnp
from jax import lax
from jax.experimental import pallas as pl
from jax.experimental.pallas import tpu as pltpu
from jax.sharding import PartitionSpec as P

C = 640
GROUP = 20
W = 64
HR = 8
POS = HR * W
QC = 160
COUNT = 2048 * GROUP
CTL = 140
MESH = pl.DeviceIdType.MESH
F32 = jnp.float32
BF16 = jnp.bfloat16


OWN = "own"
PIECE = "piece"
REST = "c"
BLOCK = "block"
CONV = "conv"
FORWARD = "fwd"
LATE = "zlate0"
EDGES = "edges"
STATS = "stats"
TIME = "time"
FIRST = "first"
HIDDEN = "hidden"
SECOND = "second"
N1 = "N1"
N2 = "N2"
FAR = "F"
MAIN = "P"
LAST = "C"
ORDER = (
    (OWN, 0, N1, MAIN, 1),
    (OWN, 0, N2, MAIN, 2),
    (OWN, 0, N1, MAIN, 2),
    (OWN, 0, N2, MAIN, 0),
    (OWN, 0, N2, LAST, 0),
    (OWN, 0, N1, MAIN, 0),
    (OWN, 0, N1, LAST, 2),
    (OWN, 0, N2, MAIN, 1),
    (STATS,),
    (OWN, 0, N1, LAST, 0),
    (OWN, 0, N2, LAST, 2),
    (TIME,),
    (OWN, 0, N2, LAST, 1),
    (PIECE, 0, N2, 2),
    (PIECE, 0, N1, 2),
    (PIECE, 0, N1, 0),
    (OWN, 0, N1, LAST, 1),
    (OWN, 1, N1, MAIN, 0),
    (PIECE, 0, N2, 1),
    (REST, 0, N1, 2),
    (PIECE, 0, N1, 1),
    (EDGES,),
    (OWN, 1, N2, MAIN, 2),
    (PIECE, 0, N2, 0),
    (OWN, 1, N1, MAIN, 1),
    (LATE,),
    (BLOCK, 0, N1, 2),
    (PIECE, 0, FAR, 0),
    (REST, 0, N1, 0),
    (OWN, 1, N1, MAIN, 2),
    (REST, 0, N2, 1),
    (PIECE, 0, FAR, 1),
    (PIECE, 0, FAR, 2),
    (OWN, 1, N2, MAIN, 0),
    (BLOCK, 0, N1, 0),
    (BLOCK, 0, N2, 1),
    (REST, 0, N1, 1),
    (OWN, 1, N2, MAIN, 1),
    (REST, 0, N2, 2),
    (REST, 0, N2, 0),
    (BLOCK, 0, N1, 1),
    (OWN, 1, N2, LAST, 2),
    (PIECE, 1, N1, 0),
    (FIRST,),
    (BLOCK, 0, N2, 0),
    (OWN, 1, N1, LAST, 2),
    (CONV, 0, N1, 0),
    (OWN, 1, N2, LAST, 1),
    (PIECE, 1, N2, 2),
    (OWN, 1, N2, LAST, 0),
    (BLOCK, 0, N2, 2),
    (CONV, 0, N1, 1),
    (OWN, 1, N1, LAST, 0),
    (OWN, 1, N1, LAST, 1),
    (CONV, 0, N1, 2),
    (BLOCK, 0, FAR, 0),
    (CONV, 0, N2, 0),
    (PIECE, 1, N1, 2),
    (PIECE, 1, N1, 1),
    (HIDDEN, N1),
    (FORWARD, N2, 2),
    (BLOCK, 0, FAR, 1),
    (FORWARD, N1, 0),
    (CONV, 0, N2, 1),
    (BLOCK, 0, FAR, 2),
    (CONV, 0, N2, 2),
    (CONV, 0, FAR, 0),
    (PIECE, 1, N2, 0),
    (HIDDEN, N2),
    (CONV, 0, FAR, 1),
    (CONV, 0, FAR, 2),
    (HIDDEN, FAR),
    (PIECE, 1, N2, 1),
    (REST, 1, N2, 1),
    (FORWARD, N1, 1),
    (REST, 1, N1, 0),
    (BLOCK, 1, N1, 0),
    (PIECE, 1, FAR, 0),
    (REST, 1, N2, 2),
    (REST, 1, N1, 2),
    (REST, 1, N2, 0),
    (REST, 1, N1, 1),
    (BLOCK, 1, N1, 1),
    (PIECE, 1, FAR, 2),
    (BLOCK, 1, N1, 2),
    (BLOCK, 1, N2, 0),
    (SECOND,),
    (PIECE, 1, FAR, 1),
    (BLOCK, 1, N2, 1),
    (CONV, 1, N1, 0),
    (CONV, 1, N1, 1),
    (CONV, 1, N1, 2),
    (BLOCK, 1, FAR, 0),
    (BLOCK, 1, FAR, 2),
    (CONV, 1, N2, 0),
    (BLOCK, 1, N2, 2),
    (CONV, 1, N2, 1),
    (BLOCK, 1, FAR, 1),
    (CONV, 1, FAR, 0),
    (CONV, 1, N2, 2),
    (CONV, 1, FAR, 1),
    (CONV, 1, FAR, 2),
)
AHEAD = {
    (0, FAR, 2),
    (0, N1, 2),
    (0, N2, 1),
    (1, FAR, 0),
    (1, FAR, 1),
    (1, FAR, 2),
    (1, N1, 0),
    (1, N1, 1),
    (1, N1, 2),
    (1, N2, 0),
    (1, N2, 1),
    (1, N2, 2),
}


def group_of(c):
    return (c * 3277) >> 16


def iota(shape, dim):
    return lax.broadcasted_iota(jnp.int32, shape, dim)


def split3(x):
    hi = x.astype(BF16).astype(F32)
    left = x - hi
    mid = left.astype(BF16).astype(F32)
    return jnp.concatenate([hi, mid, left - mid], axis=0).astype(BF16)


def exact_dot(x, m):
    out = jnp.dot(split3(x), m, preferred_element_type=F32)
    return out[0:8] + out[8:16] + out[16:24]


def silu(x):
    h = 0.5 * x
    return h + h * jnp.tanh(h)


class Links:
    def __init__(self, send, recv):
        self.send, self.recv = send, recv
        self.keys, self.started, self.count = {}, [], 0

    def slot(self, key):
        return self.keys.setdefault(key, len(self.keys))

    def prepare(self, key, src, dst, device):
        copy = pltpu.make_async_remote_copy(
            src_ref=src,
            dst_ref=dst,
            send_sem=self.send.at[self.count],
            recv_sem=self.recv.at[self.slot(key)],
            device_id=device,
            device_id_type=MESH,
        )
        self.count += 1
        self.started.append(copy)
        return copy

    def put(self, key, src, dst, device):
        self.prepare(key, src, dst, device).start()

    def get(self, key, dst, device):
        pltpu.make_async_remote_copy(
            src_ref=dst,
            dst_ref=dst,
            send_sem=self.send.at[0],
            recv_sem=self.recv.at[self.slot(key)],
            device_id=device,
            device_id_type=MESH,
        ).wait_recv()

    def drain(self):
        for copy in self.started:
            copy.wait_send()


def kernel(
    ts, freq, feats, w1, w2, b1, b2, g1, s1, g2, s2, tw, ew, zw, zb,
    outv,
    src, hid, xcat, acc, ctl, wt, group, stats, sums2, vin, shift, bias2, res, twv, ewv, zwv, fr,
    lsem, send, recv,
):
    x = lax.axis_index("rows")
    b = lax.axis_index("batch")
    branch = lax.axis_index("branch")
    core = b % 2
    zh = (b // 2) % 4
    y = b // 8
    label = (y + 2 * zh) % 4

    def along_x(by):
        return {"rows": (x + by) % 4}

    def along_batch(ny, nz, nc):
        return {"batch": (ny * 4 + nz) * 2 + nc}

    right, left, across = along_x(1), along_x(3), along_x(2)
    n1q = x + 1 - 2 * (x % 2)
    n2q = 3 - x
    n1, n2 = {"rows": n1q}, {"rows": n2q}
    up, down = along_batch((y + 1) % 4, zh, core), along_batch((y + 3) % 4, zh, core)
    front, back = along_batch(y, (zh + 1) % 4, core), along_batch(y, (zh + 3) % 4, core)
    twin = along_batch(y, zh, 1 - core)
    mate = {"branch": 1 - branch}

    barrier = pltpu.get_barrier_semaphore()
    for device in (right, left, across, up, down, front, back, twin, mate):
        pl.semaphore_signal(barrier, inc=1, device_id=device, device_id_type=MESH)

    local = {}

    def load(name, a, to):
        copy = pltpu.make_async_copy(a, to, lsem.at[len(local)])
        copy.start()
        local[name] = copy

    weights = (w1, w2)
    for t in range(5):
        load(f"feats{t}", feats.at[:, pl.ds(128 * t, 128)], src.at[t, pl.ds(W, POS), :])
    own_rows = pl.ds(pl.multiple_of(QC * x, 32), QC)
    load("fr", freq, fr)
    for i, ref in enumerate((b1, b2, g1, s1, g2, s2)):
        load(f"vec{i}", ref, vin.at[i])
    load("vec6", zb, vin.at[6, 0])

    pl.semaphore_wait(barrier, 9)
    net = Links(send, recv)
    put, get = net.put, net.get

    quarter = {"own": x, "N1": n1q, "N2": n2q, "F": (x + 2) % 4}
    side = {"N1": n1, "N2": n2}

    def piece(v, rel, u, d):
        row = pl.multiple_of(QC * quarter[rel] + 80 * core + 16 * u, 16)
        return wt.at[v, pl.ds(3 * d, 3), pl.ds(row, 16), :]

    def block(v, rel, c, d):
        row = pl.multiple_of(QC * quarter[rel] + 80 * c, 16)
        return wt.at[v, pl.ds(3 * d, 3), pl.ds(row, 80), :]

    def send_own(v, rel, kind, d):
        u = label if kind == "P" else 4
        a = weights[v].at[pl.ds(3 * d, 3), pl.ds(pl.multiple_of(80 * core + 16 * u, 16), 16), :]
        put((v, rel, kind, d), a, piece(v, "own", u, d), side[rel])

    def z_put(v, rel, d):
        ref = piece(v, rel, label, d)
        ahead = jnp.where((branch == 1) & (v == 1), 3, 1 if (v, rel, d) in AHEAD else 3)
        return net.prepare((v, rel, "Z", d), ref, ref, along_batch(y, (zh + ahead) % 4, core))

    late, passed = ([], []), [False, True]

    def forward(v, rel, d):
        ref = piece(v, rel, label, d)
        if rel == "N1" and d < 2:
            put((v, "F", "P", d), ref, ref, n2)
        if rel == "N2" and d == 2:
            put((v, "F", "P", d), ref, ref, n1)

    def on_piece(v, rel, d):
        ref = piece(v, rel, label, d)
        came = rel if rel != "F" else ("N1" if d < 2 else "N2")
        get((v, rel, "P", d), ref, side["N2" if came == "N1" else "N1"] if rel == "F" else side[rel])
        if v == 0:
            forward(v, rel, d)
        put((v, rel, "Yd", d), ref, ref, up)
        put((v, rel, "Yu", d), ref, ref, down)
        copy = z_put(v, rel, d)
        if passed[v]:
            copy.start()
        else:
            pl.when(branch == 0)(copy.start)
            late[v].append(copy)

    def z_late(v):
        passed[v] = True

        @pl.when(branch == 1)
        def _():
            for copy in late[v]:
                copy.start()

    def on_c(v, rel, d):
        ref = piece(v, rel, 4, d)
        get((v, rel, "C", d), ref, side[rel])
        if rel == "N1" and d == 0:
            put((v, "F", "C", d), ref, ref, n2)
        if rel == "N2" and d > 0:
            put((v, "F", "C", d), ref, ref, n1)

    def on_block(v, rel, d):
        if rel == "F":
            get((v, "F", "C", d), piece(v, "F", 4, d), n2 if d == 0 else n1)
        get((v, rel, "Yu", d), piece(v, rel, (label + 1) % 4, d), up)
        get((v, rel, "Yd", d), piece(v, rel, (label + 3) % 4, d), down)
        get((v, rel, "Z", d), piece(v, rel, (label + 2) % 4, d), back if (v, rel, d) in AHEAD else front)
        ref = block(v, rel, core, d)
        put((v, rel, "S", d), ref, ref, twin)

    def twin_block(v, rel, d):
        get((v, rel, "S", d), block(v, rel, 1 - core, d), twin)

    count = {"N1": 2, "N2": 1, "F": 2}

    def tile(rel, at):
        if rel == "N1":
            return jnp.where(at < 2, 0, 3)
        if rel == "N2":
            return jnp.where(at == 0, 4, jnp.where(at == 3, 0, 2))
        return (at + 2) % 4

    def tiles(rel, at):
        return pl.ds(tile(rel, at), count[rel])

    def group_matrix():
        for k in range(10):
            i = iota((64, C), 0) + 64 * k
            j = iota((64, C), 1)
            group[pl.ds(64 * k, 64), :] = jnp.where(group_of(i) == group_of(j), 1.0, 0.0).astype(BF16)

    def in_rows(total, square):
        row = iota((8, total.shape[1]), 0)
        return jnp.where(
            row == 0,
            jnp.sum(total, axis=0, keepdims=True),
            jnp.where(row == 1, jnp.sum(square, axis=0, keepdims=True), 0.0),
        )

    def moments(total):
        both = exact_dot(total, group[...]) * (1.0 / COUNT)
        mean = both[0:1]
        var = both[1:2] - mean * mean
        return mean, lax.rsqrt(var + 1e-05)

    def halo(buf, t, key):
        put((key, "top"), buf.at[t(x), pl.ds(POS, W), :], buf.at[t(x), pl.ds(0, W), :], right)
        put((key, "end"), buf.at[t(x), pl.ds(W, W), :], buf.at[t(x), pl.ds(POS + W, W), :], left)

    def wait_halo(buf, t, key):
        get((key, "top"), buf.at[t((x + 3) % 4), pl.ds(0, W), :], left)
        get((key, "end"), buf.at[t((x + 1) % 4), pl.ds(POS + W, W), :], right)

    def all_tiles(at):
        return pl.ds(0, 5)

    def activate(buf, mean, scale, shift):
        def step(i, _):
            rows = pl.ds(pl.multiple_of(W * i, W), W)
            outside = ((i == 0) & (x == 0)) | ((i == 9) & (x == 3))
            keep = jnp.where(outside, 0.0, 1.0)
            col = iota((W, 128), 0)
            for t in range(5):
                lanes = slice(128 * t, 128 * t + 128)
                v = buf[t, rows, :].astype(F32)
                a = silu((v - mean[:, lanes]) * scale[:, lanes] + shift[:, lanes]) * keep
                first = jnp.where(col == 0, 0.0, pltpu.roll(a, 1, 0))
                last = jnp.where(col == W - 1, 0.0, pltpu.roll(a, W - 1, 0))
                for k, part in enumerate((first, a, last)):
                    xcat[rows, pl.ds(C * k + 128 * t, 128)] = part.astype(BF16)
            return 0

        lax.fori_loop(0, 10, step, 0)

    def conv(v, t, n, d):
        rows = pl.ds(pl.multiple_of(128 * t, 128), 128 * n)
        rhs = jnp.concatenate([wt[v, 3 * d + k, rows, :] for k in range(3)], axis=1)
        for i in range(2):
            half = pl.ds(POS // 2 * i, POS // 2)
            lhs = xcat[pl.ds(W * d + POS // 2 * i, POS // 2), :]
            r = lax.dot_general(lhs, rhs, (((1,), (1,)), ((), ())), preferred_element_type=F32)
            for k in range(n):
                part = r[:, 128 * k : 128 * k + 128]
                acc[t + k, half, :] = part if d == 0 else acc[t + k, half, :] + part

    def add_up(values):
        total, square = 0.0, 0.0
        for k in range(values.shape[0] // 8):
            part = values[8 * k : 8 * k + 8]
            total, square = total + part, square + part * part
        return total, square

    def do_edges():
        halo(src, all_tiles, "features")

    def do_stats():
        load("tw", tw, twv)
        load("ew", ew, ewv)
        load("own0", w1, wt.at[0, :, own_rows, :])
        for t in range(5):
            local[f"feats{t}"].wait()

        def step(i, carry):
            rows = pl.ds(pl.multiple_of(W + W * i, W), W)
            new = []
            for t in range(5):
                total, square = add_up(src[t, rows, :].astype(F32))
                new += [carry[2 * t] + total, carry[2 * t + 1] + square]
            return tuple(new)

        carry = lax.fori_loop(0, HR, step, (jnp.zeros((8, 128), F32),) * 10)
        stats[x] = in_rows(jnp.concatenate(carry[0::2], axis=1), jnp.concatenate(carry[1::2], axis=1))
        group_matrix()
        for by, device in ((1, right), (2, across), (3, left)):
            put(("stats", by), stats.at[x], stats.at[x], device)
        load("own1", w2, wt.at[1, :, own_rows, :])
        load("zw", zw, zwv)

    def do_time():
        for i in range(7):
            local[f"vec{i}"].wait()
        local["fr"].wait()
        local["tw"].wait()
        local["ew"].wait()
        angle = jnp.broadcast_to(fr[...] * ts[0].astype(F32), (8, 320))
        n = jnp.floor(angle * (2.0 / math.pi) + 0.5)
        r = ((angle - n * 1.5703125) - n * 4.837512969970703e-4) - n * 7.549790126404332e-8
        turn = n + jnp.where(iota((8, 320), 1) < 160, 1.0, 0.0)
        turn = turn - 4.0 * jnp.floor(turn * 0.25)
        r2 = r * r
        sin_r = r + r * r2 * (-1.0 / 6 + r2 * (1.0 / 120 + r2 * (-1.0 / 5040 + r2 * (1.0 / 362880))))
        cos_r = 1.0 + r2 * (-0.5 + r2 * (1.0 / 24 + r2 * (-1.0 / 720 + r2 * (1.0 / 40320 - r2 * (1.0 / 3628800)))))
        waves = jnp.where(
            turn < 0.5, sin_r, jnp.where(turn < 1.5, cos_r, jnp.where(turn < 2.5, -sin_r, -cos_r))
        )
        inner = silu(exact_dot(waves, twv[...]))
        extra = vin[0] + exact_dot(inner, ewv[...])
        for t in range(5):
            shift[t] = extra[:, 128 * t : 128 * t + 128]
            bias2[t] = jnp.broadcast_to(vin[1][:, 128 * t : 128 * t + 128], (8, 128))

    def do_first():
        wait_halo(src, all_tiles, "features")
        for by, device in ((1, left), (2, across), (3, right)):
            get(("stats", by), stats.at[(x - by + 4) % 4], device)
        mean, scale = moments(stats[0] + stats[1] + stats[2] + stats[3])
        activate(src, mean, scale * vin[2], vin[3])

    def do_hidden(rel):
        for k in range(count[rel]):
            t = tile(rel, x) + k

            def step(i, carry):
                rows = pl.ds(pl.multiple_of(W * i, W), W)
                h = (acc[t, rows, :] + shift[t][0:1]).astype(BF16)
                hid[t, pl.ds(pl.multiple_of(W + W * i, W), W), :] = h
                total, square = add_up(h.astype(F32))
                return carry[0] + total, carry[1] + square

            zero = jnp.zeros((8, 128), F32)
            total, square = lax.fori_loop(0, HR, step, (zero, zero))
            sums2[x, t] = in_rows(total, square)
        halo(hid, lambda at: tiles(rel, at), ("hidden", rel))
        ref = sums2.at[x, tiles(rel, x)]
        for by, device in ((1, right), (2, across), (3, left)):
            put(("sums", rel, by), ref, ref, device)

    def do_second():
        for rel in ("N1", "N2", "F"):
            wait_halo(hid, lambda at: tiles(rel, at), ("hidden", rel))
            for by, device in ((1, left), (2, across), (3, right)):
                at = (x - by + 4) % 4
                get(("sums", rel, by), sums2.at[at, tiles(rel, at)], device)
        total = [sums2[0, t] + sums2[1, t] + sums2[2, t] + sums2[3, t] for t in range(5)]
        mean, scale = moments(jnp.concatenate(total, axis=1))
        activate(hid, mean, scale * vin[4], vin[5])

    slots = {"N1": 0, "N2": 2, "F": 3}

    def ctl_copy(rel, k, half):
        t = tile(rel, x) + k
        slot = CTL + 4 * (slots[rel] + k) + half
        ref = ctl.at[t, pl.ds(POS // 4 * half, POS // 4), :]
        return pltpu.make_async_remote_copy(
            src_ref=ref,
            dst_ref=ref,
            send_sem=send.at[slot],
            recv_sem=recv.at[slot],
            device_id=mate,
            device_id_type=MESH,
        )

    def pre(t, rows):
        own = src[t, pl.ds(W + rows.start, rows.size), :].astype(F32)
        return own + acc[t, rows, :] + bias2[t][0:1]

    def give(rel):
        @pl.when(branch == 0)
        def _():
            for k in range(count[rel]):
                t = tile(rel, x) + k
                ctl[t] = pre(t, pl.ds(0, POS)).astype(BF16)
                if rel != "F":
                    for half in range(4):
                        ctl_copy(rel, k, half).start()
            if rel == "F":
                for half in range(4):
                    for k in range(2):
                        ctl_copy(rel, k, half).start()

    def do_conv(v, rel, d):
        if rel == "N1" and d == 0:
            local[f"own{v}"].wait()
        twin_block(v, rel, d)
        conv(v, tile(rel, x), count[rel], d)
        if v == 1 and d == 2:
            give(rel)

    steps = {
        "own": send_own,
        "piece": on_piece,
        "c": on_c,
        "fwd": lambda rel, d: forward(1, rel, d),
        "block": on_block,
        "conv": do_conv,
        "zlate0": lambda: z_late(0),
        "edges": do_edges,
        "stats": do_stats,
        "time": do_time,
        "first": do_first,
        "hidden": do_hidden,
        "second": do_second,
    }
    for step in ORDER:
        steps[step[0]](*step[1:])
    local["zw"].wait()

    @pl.when(branch == 1)
    def _():
        for rel in ("N1", "N2", "F"):
            n = count[rel]
            t = tile(rel, x)

            def arrive(half):
                for k in range(n):
                    ctl_copy(rel, k, half).wait_recv()

            def step(i, _):
                rows = pl.ds(pl.multiple_of(128 * i, 128), 128)
                lhs = jnp.concatenate([ctl[t + k, rows, :] for k in range(n)], axis=1)
                rhs = zwv[pl.ds(pl.multiple_of(128 * t, 128), 128 * n), :]
                r = jnp.dot(lhs, rhs, preferred_element_type=F32)
                if rel == "N1":
                    res[rows, :] = r + vin[6]
                elif rel == "N2":
                    res[rows, :] = res[rows, :] + r
                else:
                    r = (res[rows, :] + r).astype(BF16).astype(F32)
                    for k in range(5):
                        lanes = slice(128 * k, 128 * k + 128)
                        outv[rows, pl.ds(128 * k, 128)] = (pre(k, rows) + r[:, lanes]).astype(BF16)
                return 0

            for half in range(4):
                arrive(half)
                lax.fori_loop(half, half + 1, step, 0)

    @pl.when(branch == 0)
    def _():
        for t in range(5):
            outv[:, pl.ds(128 * t, 128)] = ctl[t]
        for rel in ("N1", "N2", "F"):
            for k in range(count[rel]):
                for half in range(4):
                    ctl_copy(rel, k, half).wait_send()

    net.drain()


def body(
    timestep,
    features,
    conv1_weight,
    conv1_bias,
    conv2_weight,
    conv2_bias,
    norm1_gain,
    norm1_shift,
    norm2_gain,
    norm2_shift,
    time_weight,
    emb_weight,
    zero_weight,
    zero_bias,
):
    half = 160
    line = np.exp(-math.log(10000.0) * np.arange(half, dtype=np.float32) / np.float32(half))
    freq = jnp.asarray(np.concatenate([line, line])[None].astype(np.float32))
    hbm = pl.BlockSpec(memory_space=pltpu.HBM)
    vmem = pltpu.VMEM
    result = pl.pallas_call(
        kernel,
        out_shape=pltpu.VMEM((POS, C), BF16),
        in_specs=[pl.BlockSpec(memory_space=pltpu.SMEM)] + [hbm] * 14,
        out_specs=pl.BlockSpec(memory_space=pltpu.VMEM),
        scratch_shapes=[
            vmem((5, POS + 2 * W, 128), BF16),
            vmem((5, POS + 2 * W, 128), BF16),
            vmem((POS + 2 * W, 3 * C), BF16),
            vmem((5, POS, 128), F32),
            vmem((5, POS, 128), BF16),
            vmem((2, 9, C, C), BF16),
            vmem((C, C), BF16),
            vmem((4, 8, C), F32),
            vmem((4, 5, 8, 128), F32),
            vmem((7, 1, C), F32),
            vmem((5, 8, 128), F32),
            vmem((5, 8, 128), F32),
            vmem((POS, C), F32),
            vmem((320, 1280), BF16),
            vmem((1280, C), BF16),
            vmem((C, C), BF16),
            vmem((1, 320), F32),
            pltpu.SemaphoreType.DMA((20,)),
            pltpu.SemaphoreType.DMA((CTL + 20,)),
            pltpu.SemaphoreType.DMA((CTL + 20,)),
        ],
        compiler_params=pltpu.CompilerParams(
            collective_id=0, has_side_effects=True, vmem_limit_bytes=60 * 1024 * 1024
        ),
        name="block",
    )(
        timestep,
        freq,
        features.reshape(POS, C),
        jnp.swapaxes(conv1_weight, 3, 4).reshape(9, QC, C),
        jnp.swapaxes(conv2_weight, 3, 4).reshape(9, QC, C),
        conv1_bias,
        conv2_bias,
        norm1_gain,
        norm1_shift,
        norm2_gain,
        norm2_shift,
        time_weight[0],
        emb_weight[0],
        zero_weight,
        zero_bias,
    )
    return result.reshape(1, 1, HR, W, C)


def solution(mesh):
    placed = (
        P("batch"),
        P("batch", "branch", "rows", None, None),
        P("branch", None, None, None, "rows"),
        P("branch", None),
        P("branch", None, None, None, "rows"),
        P("branch", None),
        P("branch", None),
        P("branch", None),
        P("branch", None),
        P("branch", None),
        P("branch", None, None),
        P("branch", None, None),
        P(),
        P(),
    )
    return jax.shard_map(
        body,
        mesh=mesh,
        in_specs=placed,
        out_specs=P("batch", "branch", "rows", None, None),
        check_vma=False,
    )
```
